8 devices in a mesh: dp: 1 (over z), tp: 2 (over y), sp: 4 (over x, core).
Axes of the slice: x: 2, y: 2, z: 1, core: 2. Of those that a mesh axis runs over, the one named last changes fastest.
Arguments:
- x_in: bfloat16 [64, 2048], P('dp')
- seq_lens: int32 [64], P('dp')
- k_cache: bfloat16 [64, 256, 16, 128], P('dp', 'sp', 'tp')
- v_cache: bfloat16 [64, 256, 16, 128], P('dp', 'sp', 'tp')
- ln1_gain: float32 [2048], replicated
- w_qkv: bfloat16 [2048, 3, 16, 128], P(None, None, 'tp')
- w_out: bfloat16 [16, 128, 2048], P('tp')
- ln2_gain: float32 [2048], replicated
- w_up: bfloat16 [2048, 8192], P(None, 'tp')
- w_down: bfloat16 [8192, 2048], P('tp')
Outputs:
- output 1: bfloat16 [64, 2048], P('dp')
- output 2: bfloat16 [64, 256, 16, 128], P('dp', 'sp', 'tp')
- output 3: bfloat16 [64, 256, 16, 128], P('dp', 'sp', 'tp')
All inputs are finite; a program needn't handle non-finite values.
Results may differ from the reference program's by a relative error of at most 0.00568629.
Values sent between devices are 32-bit elements.
A program may use at most 1 GiB of HBM per device.

```python
import jax
import jax.numpy as jnp
from jax import lax

BATCH = 64
CACHE_LEN = 256
BLOCK_LEN = 64
D = 2048
HEADS = 16
HEAD = 128
FF = 8192
PLANT_GAP = 64

NUM_BLOCKS = CACHE_LEN // BLOCK_LEN
LN_EPS = 1e-5
ALIBI_CAP = 256.0


def layer_norm(x_f32, gain):
    mean = jnp.mean(x_f32, axis=-1, keepdims=True)
    centred = x_f32 - mean
    variance = jnp.mean(centred * centred, axis=-1, keepdims=True)
    return centred * lax.rsqrt(variance + LN_EPS) * gain


def alibi_slopes():
    return jnp.exp2(-8.0 * (jnp.arange(HEADS).astype(jnp.float32) + 1.0) / HEADS)


def setup_inputs(seed: int = 0, part: int = 0) -> dict:
    root = jax.random.key(seed)
    shared = jax.random.split(root, 6)
    own = jax.random.split(jax.random.fold_in(root, part), 7)
    x_in = jax.random.normal(own[0], (BATCH, D), jnp.float32).astype(jnp.bfloat16)
    ln1_gain = jax.random.uniform(shared[0], (D,), jnp.float32, minval=0.5, maxval=1.5)
    w_qkv = (jax.random.normal(shared[1], (D, 3, HEADS, HEAD), jnp.float32) * D ** -0.5).astype(jnp.bfloat16)
    w_out = (jax.random.normal(shared[2], (HEADS, HEAD, D), jnp.float32) * D ** -0.5).astype(jnp.bfloat16)
    ln2_gain = jax.random.uniform(shared[3], (D,), jnp.float32, minval=0.5, maxval=1.5)
    w_up = (jax.random.normal(shared[4], (D, FF), jnp.float32) * D ** -0.5).astype(jnp.bfloat16)
    w_down = (jax.random.normal(shared[5], (FF, D), jnp.float32) * FF ** -0.5).astype(jnp.bfloat16)
    seq_lens = jax.random.randint(own[1], (BATCH,), 1, CACHE_LEN)
    longest = jax.random.randint(own[2], (), 0, BATCH)
    seq_lens = jnp.where(jnp.arange(BATCH) == longest, CACHE_LEN - 1, seq_lens).astype(jnp.int32)
    normed = layer_norm(x_in.astype(jnp.float32), ln1_gain).astype(jnp.bfloat16)
    query = jnp.dot(normed, w_qkv[:, 0].reshape(D, D), preferred_element_type=jnp.float32)
    query = query.astype(jnp.bfloat16).astype(jnp.float32).reshape(BATCH, HEADS, HEAD)
    offsets = jax.random.randint(own[3], (BATCH, CACHE_LEN // PLANT_GAP, 1), 0, PLANT_GAP)
    slot_pos = jnp.arange(CACHE_LEN)
    planted = (jnp.arange(PLANT_GAP)[None, None, :] == offsets).reshape(BATCH, CACHE_LEN)
    planted = planted & (slot_pos[None, :] < seq_lens[:, None])
    gumbel_u = jax.random.uniform(own[4], (BATCH, CACHE_LEN, HEADS), jnp.float32, minval=1e-6, maxval=1.0)
    bonus = 4.0 - 1.5 * jnp.log(-jnp.log(gumbel_u))
    distance = (seq_lens[:, None] - slot_pos[None, :]).astype(jnp.float32)
    target = jnp.minimum(alibi_slopes()[None, None, :] * distance[:, :, None], ALIBI_CAP) + bonus

    def make_keys(args):
        seq_key, q_row, target_row, planted_row = args
        k_rand = jax.random.normal(seq_key, (CACHE_LEN, HEADS, HEAD), jnp.float32)
        along = jnp.einsum("hk,thk->th", q_row, k_rand)
        coef = (target_row * HEAD ** 0.5 - along) / jnp.sum(q_row * q_row, axis=-1)[None, :]
        lifted = k_rand + coef[:, :, None] * q_row[None, :, :]
        return jnp.where(planted_row[:, None, None], lifted, k_rand).astype(jnp.bfloat16)

    def make_values(seq_key):
        return jax.random.normal(seq_key, (CACHE_LEN, HEADS, HEAD), jnp.float32).astype(jnp.bfloat16)

    k_cache = lax.map(make_keys, (jax.random.split(own[5], BATCH), query, target, planted))
    v_cache = lax.map(make_values, jax.random.split(own[6], BATCH))
    return {"x_in": x_in, "seq_lens": seq_lens, "k_cache": k_cache, "v_cache": v_cache, "ln1_gain": ln1_gain, "w_qkv": w_qkv, "w_out": w_out, "ln2_gain": ln2_gain, "w_up": w_up, "w_down": w_down}


def reference(x_in, seq_lens, k_cache, v_cache, ln1_gain, w_qkv, w_out, ln2_gain, w_up, w_down):
    normed = layer_norm(x_in.astype(jnp.float32), ln1_gain).astype(jnp.bfloat16)
    qkv_proj = jnp.dot(normed, w_qkv.reshape(D, 3 * D), preferred_element_type=jnp.float32)
    qkv_proj = qkv_proj.astype(jnp.bfloat16).reshape(BATCH, 3, HEADS, HEAD)
    slot_pos = jnp.arange(CACHE_LEN)
    slot_hit = (slot_pos[None, :] == seq_lens[:, None])[:, :, None, None]
    k_next = jnp.where(slot_hit, qkv_proj[:, 1][:, None], k_cache)
    v_next = jnp.where(slot_hit, qkv_proj[:, 2][:, None], v_cache)
    slopes = alibi_slopes()

    def attend(args):
        q_row, k_seq, v_seq, length = args
        q_f32 = q_row.astype(jnp.float32)

        def block_scores(k_block):
            return jnp.einsum("hk,thk->ht", q_f32, k_block.astype(jnp.float32))

        scores = lax.map(block_scores, k_seq.reshape(NUM_BLOCKS, BLOCK_LEN, HEADS, HEAD))
        scores = jnp.transpose(scores, (1, 0, 2)).reshape(HEADS, CACHE_LEN) * HEAD ** -0.5
        scores = scores - slopes[:, None] * (length - slot_pos).astype(jnp.float32)[None, :]
        scores = jnp.where((slot_pos <= length)[None, :], scores, -jnp.inf)
        row_max = jnp.max(scores, axis=1, keepdims=True)
        weights = jnp.exp(scores - row_max)
        row_sum = jnp.sum(weights, axis=1)
        weights_b = weights.astype(jnp.bfloat16).astype(jnp.float32)
        weights_b = jnp.transpose(weights_b.reshape(HEADS, NUM_BLOCKS, BLOCK_LEN), (1, 0, 2))

        def block_sum(carry, block_pair):
            w_block, v_block = block_pair
            return carry + jnp.einsum("ht,thk->hk", w_block, v_block.astype(jnp.float32)), None

        summed, _ = lax.scan(block_sum, jnp.zeros((HEADS, HEAD), jnp.float32), (weights_b, v_seq.reshape(NUM_BLOCKS, BLOCK_LEN, HEADS, HEAD)))
        return summed / row_sum[:, None]

    attended = lax.map(attend, (qkv_proj[:, 0], k_next, v_next, seq_lens))
    attended = attended.astype(jnp.bfloat16).reshape(BATCH, D)
    residual = x_in.astype(jnp.float32) + jnp.dot(attended, w_out.reshape(D, D), preferred_element_type=jnp.float32)
    normed_mid = layer_norm(residual, ln2_gain).astype(jnp.bfloat16)
    hidden = jax.nn.gelu(jnp.dot(normed_mid, w_up, preferred_element_type=jnp.float32), approximate=False).astype(jnp.bfloat16)
    x_out = (residual + jnp.dot(hidden, w_down, preferred_element_type=jnp.float32)).astype(jnp.bfloat16)
    return (x_out, k_next, v_next)
```

```python
import functools

import jax
import jax.numpy as jnp
from jax import lax
from jax.experimental import pallas as pl
from jax.experimental.pallas import tpu as pltpu
from jax.sharding import PartitionSpec as P

LN_EPS = 1e-5
NEG = -1e30
F32 = jnp.float32
BF16 = jnp.bfloat16
MESH = pl.DeviceIdType.MESH

B = 64
D = 2048
NH = 8
HD = 128
T = 64
NQ = 2 * D
CH = 8
CP = 32 // CH
FH = 2048
NUP = 4
NOC = 2


def layer_norm(x_f32, gain):
    mean = jnp.mean(x_f32, axis=-1, keepdims=True)
    centred = x_f32 - mean
    variance = jnp.mean(centred * centred, axis=-1, keepdims=True)
    return centred * lax.rsqrt(variance + LN_EPS) * gain


def attend_kernel(x_hbm, lens_hbm, g_hbm, k_hbm, v_hbm, w_hbm, ko_hbm, vo_hbm, o_ref,
                  x_buf, g_buf, lens, w_buf, k_buf, v_buf, lhs, q_s, k_s, v_s,
                  small_sem, w_sem, kin_sem, vin_sem, kout_sem, vout_sem):
    small = [pltpu.make_async_copy(x_hbm, x_buf, small_sem.at[0]),
             pltpu.make_async_copy(g_hbm, g_buf, small_sem.at[1]),
             pltpu.make_async_copy(lens_hbm, lens, small_sem.at[2])]
    for c in small:
        c.start()
    w_copy = [pltpu.make_async_copy(w_hbm.at[:, i], w_buf.at[i], w_sem.at[i]) for i in range(12)]
    for c in w_copy:
        c.start()

    def kv_in(i):
        rows = pl.ds(i * CP, CP)
        return (pltpu.make_async_copy(k_hbm.at[:, rows], k_buf.at[:, rows], kin_sem.at[i]),
                pltpu.make_async_copy(v_hbm.at[:, rows], v_buf.at[:, rows], vin_sem.at[i]))

    def kv_out(i):
        rows = pl.ds(i * CP, CP)
        return (pltpu.make_async_copy(k_buf.at[:, rows], ko_hbm.at[:, rows], kout_sem.at[i]),
                pltpu.make_async_copy(v_buf.at[:, rows], vo_hbm.at[:, rows], vout_sem.at[i]))

    for i in range(CH):
        for c in kv_in(i):
            c.start()

    for c in small:
        c.wait()
    normed = layer_norm(x_buf[...].astype(F32), g_buf[...]).astype(BF16)
    spread = (lax.broadcasted_iota(jnp.int32, (128, 256), 1) // 2
              == lax.broadcasted_iota(jnp.int32, (128, 256), 0)).astype(BF16)
    odd = lax.broadcasted_iota(jnp.int32, (B, 256), 1) % 2 == 1
    for i in range(D // 128):
        twice = jnp.dot(normed[:, i * 128:(i + 1) * 128], spread, preferred_element_type=F32)
        lhs[0:B, i * 256:(i + 1) * 256] = jnp.where(odd, 0.0, twice).astype(BF16)
        lhs[B:2 * B, i * 256:(i + 1) * 256] = jnp.where(odd, twice, 0.0).astype(BF16)

    w_flat = w_buf.reshape(12, NQ, HD)
    for i in range(0, 12, 2):
        w_copy[i].wait()
        w_copy[i + 1].wait()
        two = jnp.concatenate([w_flat[i], w_flat[i + 1]], axis=1)
        res = jnp.dot(lhs[...], two, preferred_element_type=F32)
        for n in range(2):
            part, pair = divmod(i + n, 4)
            for parity in range(2):
                h = 2 * pair + parity
                val = res[parity * B:(parity + 1) * B, n * HD:(n + 1) * HD]
                if part == 0:
                    base = (h // 4) * 8 + h % 4
                    q_s[pl.ds(base, 32, stride=16), :] = val[0:32]
                    q_s[pl.ds(base + 4, 32, stride=16), :] = val[32:64]
                else:
                    (k_s if part == 1 else v_s)[pl.ds(h, B, stride=NH), :] = val

    sp = lax.axis_index("sp")
    tp = lax.axis_index("tp")
    row = lax.broadcasted_iota(jnp.int32, (16, 1), 0)
    head = (row // 8) * 4 + row % 4
    slope = jnp.exp2(-8.0 * (tp * NH + head + 1).astype(F32) / (2 * NH))
    col = lax.broadcasted_iota(jnp.int32, (16, NH * T), 1)
    own_head = col % NH == (lax.broadcasted_iota(jnp.int32, (16, NH * T), 0) // 8) * 4 \
        + lax.broadcasted_iota(jnp.int32, (16, NH * T), 0) % 4
    pos = sp * T + col // NH
    pos = jnp.where(own_head, pos, 1 << 20)
    second = row % 8 >= 4
    second_q = lax.broadcasted_iota(jnp.int32, (16, HD), 0) % 8 >= 4
    second_o = lax.broadcasted_iota(jnp.int32, (8, HD), 0) >= 4
    upper = lax.broadcasted_iota(jnp.int32, (16, HD), 0) >= 8
    lane = lax.broadcasted_iota(jnp.int32, (16, HD), 1)

    def insert(buf, new, half, j):
        b = half * 32 + j
        slot = lens[b] - sp * T
        held = jnp.logical_and(slot >= 0, slot < T)
        at = jnp.clip(slot, 0, T - 1)
        rows = pl.ds(pl.multiple_of((at // 2) * 16, 16), 16)
        fresh = new[pl.ds(pl.multiple_of(b * NH, NH), NH), :]
        fresh = jnp.concatenate([fresh, fresh], axis=0)
        keep = jnp.where(held, at % 2, 2)
        old = buf[half, j, rows, :].astype(F32)
        mine = upper.astype(jnp.int32) == keep
        buf[half, j, rows, :] = jnp.where(mine, fresh, old).astype(BF16)

    def chunk(i, stats):
        for c in kv_in(i):
            c.wait()
        for n in range(CP):
            for half in range(2):
                insert(k_buf, k_s, half, i * CP + n)
                insert(v_buf, v_s, half, i * CP + n)
        scores = []
        for n in range(CP):
            j = i * CP + n
            q = q_s[pl.ds(pl.multiple_of(j * 16, 16), 16), :]
            q2 = jnp.concatenate([jnp.where(second_q, 0.0, q), jnp.where(second_q, q, 0.0)], axis=1).astype(BF16)
            k2 = jnp.concatenate([k_buf[0, j], k_buf[1, j]], axis=1)
            scores.append(lax.dot_general(q2, k2, (((1,), (1,)), ((), ())), preferred_element_type=F32))
        weights = []
        for n in range(CP):
            j = i * CP + n
            length = jnp.where(second, lens[32 + j], lens[j])
            valid = pos <= length
            s = scores[n] * HD ** -0.5 - slope * (length - pos).astype(F32)
            s = jnp.where(valid, s, NEG)
            top = jnp.max(s, axis=1, keepdims=True)
            p = jnp.where(valid, jnp.exp(s - top), 0.0)
            total = jnp.sum(p, axis=1, keepdims=True)
            weights.append(p.astype(BF16))
            stats = jnp.where(lane == j, top, jnp.where(lane == 64 + j, total, stats))
        for n in range(CP):
            j = i * CP + n
            v2 = jnp.concatenate([v_buf[0, j], v_buf[1, j]], axis=1)
            o = jnp.dot(weights[n], v2, preferred_element_type=F32)
            for c in range(2):
                piece = jnp.where(second_o, o[c * 8:(c + 1) * 8, HD:], o[c * 8:(c + 1) * 8, :HD])
                o_ref[c, i // (CH // 2), pl.ds(pl.multiple_of((j % 16) * 8, 8), 8), :] = piece
        for c in kv_out(i):
            c.start()
        return stats

    stats = lax.fori_loop(0, CH, chunk, jnp.zeros((16, HD), F32))
    for c in range(2):
        for x in range(2):
            o_ref[c, x, 128:136, :] = stats[c * 8:(c + 1) * 8]
    for i in range(CH):
        for c in kv_out(i):
            c.wait()


def rest_kernel(o_ref, x_hbm, g_hbm, wo_hbm, wu_hbm, wd_hbm, out_ref,
                x_buf, g_buf, wo_buf, wu_buf, wd_buf, o_recv, att, a_send, a_recv, y_send, y_recv, r_buf,
                hid, d_send, d_recv, z_send, z_recv, f_send, f_recv,
                in_sem, wo_sem, wu_sem, wd_sem, o_ss, o_rs, a_ss, a_rs, y_ss, y_rs, r_ss, r_rs,
                d_ss, d_rs, z_ss, z_rs, f_ss, f_rs):
    sp = lax.axis_index("sp")
    tp = lax.axis_index("tp")
    x = sp // 2
    c = sp % 2
    core = {"sp": x * 2 + (1 - c)}
    flip = {"sp": (1 - x) * 2 + c}
    other_tp = {"tp": 1 - tp}
    half = D // 2
    w = half // NOC

    def remote(src, dst, ss, rs, dev):
        return pltpu.make_async_remote_copy(src_ref=src, dst_ref=dst, send_sem=ss, recv_sem=rs, device_id=dev,
                                            device_id_type=MESH)

    wo_copy, wd_copy = [], []
    for n in range(2):
        cols = pl.ds(pl.multiple_of(((1 - c) if n == 0 else c) * half, half), half)
        wo_copy.append(pltpu.make_async_copy(wo_hbm.at[pl.ds(pl.multiple_of(c * 512, 512), 512), cols], wo_buf.at[n],
                                             wo_sem.at[n]))
        for k in range(NOC):
            cols = pl.ds(pl.multiple_of(((1 - c) if n == 0 else c) * half + k * w, w), w)
            wd_copy.append(pltpu.make_async_copy(wd_hbm.at[pl.ds(pl.multiple_of(c * FH, FH), FH), cols],
                                                 wd_buf.at[n * NOC + k], wd_sem.at[n * NOC + k]))
    wu_copy = [pltpu.make_async_copy(wu_hbm.at[:, pl.ds(pl.multiple_of(c * FH + k * (FH // NUP), FH // NUP), FH // NUP)],
                                     wu_buf.at[k], wu_sem.at[k]) for k in range(NUP)]
    in_copy = [pltpu.make_async_copy(g_hbm, g_buf, in_sem.at[0])]
    for n in range(2):
        in_copy.append(pltpu.make_async_copy(
            x_hbm.at[pl.ds(pl.multiple_of(n * 32 + x * 16, 16), 16), pl.ds(pl.multiple_of(c * half, half), half)],
            x_buf.at[n], in_sem.at[1 + n]))
    for cp in wo_copy + in_copy + wu_copy + wd_copy:
        cp.start()

    barrier = pltpu.get_barrier_semaphore()
    for rel in range(1, 4):
        pl.semaphore_signal(barrier, inc=1, device_id={"sp": (sp + rel) % 4}, device_id_type=MESH)
    pl.semaphore_signal(barrier, inc=1, device_id=other_tp, device_id_type=MESH)
    pl.semaphore_wait(barrier, 4)

    o_copy = []
    for rel in range(1, 4):
        peer = (sp + rel) % 4
        o_copy.append(remote(o_ref.at[peer % 2, peer // 2], o_recv.at[rel - 1], o_ss.at[rel - 1], o_rs.at[rel - 1],
                             {"sp": peer}))
    for cp in o_copy:
        cp.start()
    for cp in o_copy:
        cp.wait()
    parts = [o_ref.at[c, x]] + [o_recv.at[n] for n in range(3)]
    shift = (HD - 16 * x) % HD
    tops = [pltpu.roll(p[128:136, :], shift, 1) for p in parts]
    sums = [pltpu.roll(t, 64, 1) for t in tops]
    top = functools.reduce(jnp.maximum, tops)
    scale = [jnp.exp(t - top) for t in tops]
    total = functools.reduce(jnp.add, [a * s for a, s in zip(scale, sums)])
    scale = [a / total for a in scale]
    for j in range(16):
        acc = None
        for a, p in zip(scale, parts):
            term = p[j * 8:(j + 1) * 8, :] * a[:, j:j + 1]
            acc = term if acc is None else acc + term
        att[j * 8:(j + 1) * 8, :] = acc

    rows = []
    for bb in range(2):
        rows.append(jnp.concatenate([att[pl.ds(bb * 4 + h, 16, stride=8), :] for h in range(4)], axis=1))
    attended = jnp.concatenate(rows, axis=0).astype(BF16)
    wo_copy[0].wait()
    a_copy = []
    for k in range(NOC):
        a_send[k] = jnp.dot(attended, wo_buf[0, :, k * w:(k + 1) * w], preferred_element_type=F32)
        a_copy.append(remote(a_send.at[k], a_recv.at[k], a_ss.at[k], a_rs.at[k], core))
        a_copy[k].start()
    wo_copy[1].wait()
    own = [jnp.dot(attended, wo_buf[1, :, k * w:(k + 1) * w], preferred_element_type=F32) for k in range(NOC)]
    y_copy = []
    for k in range(NOC):
        a_copy[k].wait()
        y_send[k] = own[k] + a_recv[k]
        y_copy.append(remote(y_send.at[k], y_recv.at[k], y_ss.at[k], y_rs.at[k], other_tp))
        y_copy[k].start()
    for cp in in_copy:
        cp.wait()
    x_in = jnp.concatenate([x_buf[0], x_buf[1]], axis=0).astype(F32)
    r_copy = []
    for k in range(NOC):
        y_copy[k].wait()
        r_buf[c, k] = x_in[:, k * w:(k + 1) * w] + (y_send[k] + y_recv[k])
        r_copy.append(remote(r_buf.at[c, k], r_buf.at[c, k], r_ss.at[k], r_rs.at[k], core))
        r_copy[k].start()
    for cp in r_copy:
        cp.wait()

    res = jnp.concatenate([r_buf[n, k] for n in range(2) for k in range(NOC)], axis=1)
    normed = layer_norm(res, g_buf[...]).astype(BF16)
    fw = FH // NUP
    for k in range(NUP):
        wu_copy[k].wait()
        u = jnp.dot(normed, wu_buf[k], preferred_element_type=F32)
        hid[:, k * fw:(k + 1) * fw] = (0.5 * u * (1.0 + lax.erf(u * 0.5 ** 0.5))).astype(BF16)
    d_copy = []
    for k in range(NOC):
        wd_copy[k].wait()
        d_send[k] = jnp.dot(hid[...], wd_buf[k], preferred_element_type=F32)
        d_copy.append(remote(d_send.at[k], d_recv.at[k], d_ss.at[k], d_rs.at[k], core))
        d_copy[k].start()
    z_copy = []
    for k in range(NOC):
        wd_copy[NOC + k].wait()
        mine = jnp.dot(hid[...], wd_buf[NOC + k], preferred_element_type=F32)
        d_copy[k].wait()
        z_send[k] = mine + d_recv[k]
        z_copy.append(remote(z_send.at[k], z_recv.at[k], z_ss.at[k], z_rs.at[k], other_tp))
        z_copy[k].start()

    def put(block, where, cc, k):
        for n in range(2):
            out_ref[pl.ds(pl.multiple_of(n * 32 + where * 16, 16), 16),
                    pl.ds(pl.multiple_of(cc * half + k * w, w), w)] = block[n * 16:(n + 1) * 16].astype(BF16)

    near, far, fwd = [], [], []
    for k in range(NOC):
        z_copy[k].wait()
        val = r_buf[c, k] + (z_send[k] + z_recv[k])
        f_send[k] = val
        far.append(remote(f_send.at[k], f_recv.at[1, k], f_ss.at[1, k], f_rs.at[1, k], flip))
        far[k].start()
        near.append(remote(f_send.at[k], f_recv.at[0, k], f_ss.at[0, k], f_rs.at[0, k], core))
        near[k].start()
        put(val, x, c, k)
    for k in range(NOC):
        far[k].wait()
        fwd.append(remote(f_recv.at[1, k], f_recv.at[2, k], f_ss.at[2, k], f_rs.at[2, k], core))
        fwd[k].start()
        put(f_recv[1, k], 1 - x, c, k)
    for k in range(NOC):
        near[k].wait()
        put(f_recv[0, k], x, 1 - c, k)
    for k in range(NOC):
        fwd[k].wait()
        put(f_recv[2, k], 1 - x, 1 - c, k)


def solution(mesh):
    def hbm(a):
        return pltpu.with_memory_space_constraint(a, pltpu.HBM)

    in_hbm = pl.BlockSpec(memory_space=pltpu.HBM)
    in_vmem = pl.BlockSpec(memory_space=pltpu.VMEM)
    dma = pltpu.SemaphoreType.DMA

    def local_layer(x_in, seq_lens, k_cache, v_cache, ln1_gain, w_qkv, w_out, ln2_gain, w_up, w_down):
        caches = [hbm(a.reshape(2, B // 2, T * NH, HD)) for a in (k_cache, v_cache)]
        cache_type = jax.ShapeDtypeStruct((2, B // 2, T * NH, HD), BF16)
        k_next, v_next, parts = pl.pallas_call(
            attend_kernel,
            out_shape=[cache_type, cache_type, jax.ShapeDtypeStruct((2, 2, 136, HD), F32)],
            in_specs=[in_hbm] * 6,
            out_specs=[in_hbm, in_hbm, in_vmem],
            scratch_shapes=[
                pltpu.VMEM((B, D), BF16), pltpu.VMEM((1, D), F32), pltpu.SMEM((B,), jnp.int32),
                pltpu.VMEM((12, D, 2, HD), BF16),
                pltpu.VMEM((2, B // 2, T * NH, HD), BF16), pltpu.VMEM((2, B // 2, T * NH, HD), BF16),
                pltpu.VMEM((2 * B, NQ), BF16),
                pltpu.VMEM((B * NH, HD), F32), pltpu.VMEM((B * NH, HD), F32), pltpu.VMEM((B * NH, HD), F32),
                dma((3,)), dma((12,)), dma((CH,)), dma((CH,)), dma((CH,)), dma((CH,)),
            ],
            compiler_params=pltpu.CompilerParams(vmem_limit_bytes=44 * 1024 * 1024),
            name="attend",
        )(hbm(x_in), hbm(seq_lens), hbm(ln1_gain.reshape(1, D)), *caches, hbm(w_qkv.reshape(D, 12, 2, HD)))
        w = D // 2 // NOC
        x_out = pl.pallas_call(
            rest_kernel,
            out_shape=jax.ShapeDtypeStruct((B, D), BF16),
            in_specs=[in_vmem] + [in_hbm] * 5,
            out_specs=in_vmem,
            scratch_shapes=[
                pltpu.VMEM((2, 16, D // 2), BF16), pltpu.VMEM((1, D), F32),
                pltpu.VMEM((2, 512, D // 2), BF16), pltpu.VMEM((NUP, D, FH // NUP), BF16),
                pltpu.VMEM((2 * NOC, FH, w), BF16),
                pltpu.VMEM((3, 136, HD), F32), pltpu.VMEM((128, HD), F32),
                pltpu.VMEM((NOC, 32, w), F32), pltpu.VMEM((NOC, 32, w), F32),
                pltpu.VMEM((NOC, 32, w), F32), pltpu.VMEM((NOC, 32, w), F32),
                pltpu.VMEM((2, NOC, 32, w), F32),
                pltpu.VMEM((32, FH), BF16),
                pltpu.VMEM((NOC, 32, w), F32), pltpu.VMEM((NOC, 32, w), F32),
                pltpu.VMEM((NOC, 32, w), F32), pltpu.VMEM((NOC, 32, w), F32),
                pltpu.VMEM((NOC, 32, w), F32), pltpu.VMEM((3, NOC, 32, w), F32),
                dma((3,)), dma((2,)), dma((NUP,)), dma((2 * NOC,)), dma((3,)), dma((3,)),
                dma((NOC,)), dma((NOC,)), dma((NOC,)), dma((NOC,)), dma((NOC,)), dma((NOC,)),
                dma((NOC,)), dma((NOC,)), dma((NOC,)), dma((NOC,)), dma((3, NOC)), dma((3, NOC)),
            ],
            compiler_params=pltpu.CompilerParams(vmem_limit_bytes=32 * 1024 * 1024, collective_id=0,
                                                 has_side_effects=True),
            name="rest",
        )(parts, hbm(x_in), hbm(ln2_gain.reshape(1, D)), hbm(w_out.reshape(NH * HD, D)), hbm(w_up), hbm(w_down))
        return x_out, k_next.reshape(k_cache.shape), v_next.reshape(v_cache.shape)

    cache_spec = P("dp", "sp", "tp", None)
    in_specs = (P("dp", None), P("dp"), cache_spec, cache_spec, P(None), P(None, None, "tp", None), P("tp", None, None), P(None), P(None, "tp"), P("tp", None))
    out_specs = (P("dp", None), cache_spec, cache_spec)
    return jax.shard_map(local_layer, mesh=mesh, in_specs=in_specs, out_specs=out_specs, check_vma=False)
```

```python
import functools

import jax
import jax.numpy as jnp
from jax import lax
from jax.experimental import pallas as pl
from jax.experimental.pallas import tpu as pltpu
from jax.sharding import PartitionSpec as P

LN_EPS = 1e-5
NEG = -1e30
F32 = jnp.float32
BF16 = jnp.bfloat16
MESH = pl.DeviceIdType.MESH

B = 64
D = 2048
NH = 8
HD = 128
T = 64
NQ = 2 * D
CH = 8
CP = 32 // CH
FH = 2048
NUP = 4
NOC = 2


def layer_norm(x_f32, gain):
    mean = jnp.mean(x_f32, axis=-1, keepdims=True)
    centred = x_f32 - mean
    variance = jnp.mean(centred * centred, axis=-1, keepdims=True)
    return centred * lax.rsqrt(variance + LN_EPS) * gain


def prepare_kernel(x_hbm, g_hbm, w_hbm, w_out, lhs, x_buf, g_buf, small_sem, w_sem):
    small = [pltpu.make_async_copy(x_hbm, x_buf, small_sem.at[0]),
             pltpu.make_async_copy(g_hbm, g_buf, small_sem.at[1])]
    w_copy = [pltpu.make_async_copy(w_hbm.at[:, i], w_out.at[i], w_sem.at[i]) for i in range(12)]
    for c in small + w_copy:
        c.start()
    for c in small:
        c.wait()
    normed = layer_norm(x_buf[...].astype(F32), g_buf[...]).astype(BF16)
    spread = (lax.broadcasted_iota(jnp.int32, (128, 256), 1) // 2
              == lax.broadcasted_iota(jnp.int32, (128, 256), 0)).astype(BF16)
    odd = lax.broadcasted_iota(jnp.int32, (B, 256), 1) % 2 == 1
    for i in range(D // 128):
        twice = jnp.dot(normed[:, i * 128:(i + 1) * 128], spread, preferred_element_type=F32)
        lhs[0:B, i * 256:(i + 1) * 256] = jnp.where(odd, 0.0, twice).astype(BF16)
        lhs[B:2 * B, i * 256:(i + 1) * 256] = jnp.where(odd, twice, 0.0).astype(BF16)
    for c in w_copy:
        c.wait()


def attend_kernel(lhs, w_ref, lens_hbm, k_hbm, v_hbm, ko_hbm, vo_hbm, o_ref,
                  lens, k_buf, v_buf, q_s, k_s, v_s,
                  small_sem, kin_sem, vin_sem, kout_sem, vout_sem):
    lens_copy = pltpu.make_async_copy(lens_hbm, lens, small_sem)
    lens_copy.start()

    def kv_in(i):
        rows = pl.ds(i * CP, CP)
        return (pltpu.make_async_copy(k_hbm.at[:, rows], k_buf.at[:, rows], kin_sem.at[i]),
                pltpu.make_async_copy(v_hbm.at[:, rows], v_buf.at[:, rows], vin_sem.at[i]))

    def kv_out(i):
        rows = pl.ds(i * CP, CP)
        return (pltpu.make_async_copy(k_buf.at[:, rows], ko_hbm.at[:, rows], kout_sem.at[i]),
                pltpu.make_async_copy(v_buf.at[:, rows], vo_hbm.at[:, rows], vout_sem.at[i]))

    for i in range(CH):
        for c in kv_in(i):
            c.start()

    for i in range(0, 12, 2):
        two = jnp.concatenate([w_ref[i], w_ref[i + 1]], axis=1)
        res = jnp.dot(lhs[...], two, preferred_element_type=F32)
        for n in range(2):
            part, pair = divmod(i + n, 4)
            for parity in range(2):
                h = 2 * pair + parity
                val = res[parity * B:(parity + 1) * B, n * HD:(n + 1) * HD]
                if part == 0:
                    base = (h // 4) * 8 + h % 4
                    q_s[pl.ds(base, 32, stride=16), :] = val[0:32]
                    q_s[pl.ds(base + 4, 32, stride=16), :] = val[32:64]
                else:
                    (k_s if part == 1 else v_s)[pl.ds(h, B, stride=NH), :] = val
    lens_copy.wait()

    sp = lax.axis_index("sp")
    tp = lax.axis_index("tp")
    row = lax.broadcasted_iota(jnp.int32, (16, 1), 0)
    head = (row // 8) * 4 + row % 4
    slope = jnp.exp2(-8.0 * (tp * NH + head + 1).astype(F32) / (2 * NH))
    col = lax.broadcasted_iota(jnp.int32, (16, NH * T), 1)
    own_head = col % NH == (lax.broadcasted_iota(jnp.int32, (16, NH * T), 0) // 8) * 4 \
        + lax.broadcasted_iota(jnp.int32, (16, NH * T), 0) % 4
    pos = sp * T + col // NH
    pos = jnp.where(own_head, pos, 1 << 20)
    second = row % 8 >= 4
    second_q = lax.broadcasted_iota(jnp.int32, (16, HD), 0) % 8 >= 4
    second_o = lax.broadcasted_iota(jnp.int32, (8, HD), 0) >= 4
    upper = lax.broadcasted_iota(jnp.int32, (16, HD), 0) >= 8
    lane = lax.broadcasted_iota(jnp.int32, (16, HD), 1)

    def insert(buf, new, half, j):
        b = half * 32 + j
        slot = lens[b] - sp * T
        held = jnp.logical_and(slot >= 0, slot < T)
        at = jnp.clip(slot, 0, T - 1)
        rows = pl.ds(pl.multiple_of((at // 2) * 16, 16), 16)
        fresh = new[pl.ds(pl.multiple_of(b * NH, NH), NH), :]
        fresh = jnp.concatenate([fresh, fresh], axis=0)
        keep = jnp.where(held, at % 2, 2)
        old = buf[half, j, rows, :].astype(F32)
        mine = upper.astype(jnp.int32) == keep
        buf[half, j, rows, :] = jnp.where(mine, fresh, old).astype(BF16)

    def chunk(i, stats):
        for c in kv_in(i):
            c.wait()
        for n in range(CP):
            for half in range(2):
                insert(k_buf, k_s, half, i * CP + n)
                insert(v_buf, v_s, half, i * CP + n)
        scores = []
        for n in range(CP):
            j = i * CP + n
            q = q_s[pl.ds(pl.multiple_of(j * 16, 16), 16), :]
            q2 = jnp.concatenate([jnp.where(second_q, 0.0, q), jnp.where(second_q, q, 0.0)], axis=1).astype(BF16)
            k2 = jnp.concatenate([k_buf[0, j], k_buf[1, j]], axis=1)
            scores.append(lax.dot_general(q2, k2, (((1,), (1,)), ((), ())), preferred_element_type=F32))
        weights = []
        for n in range(CP):
            j = i * CP + n
            length = jnp.where(second, lens[32 + j], lens[j])
            valid = pos <= length
            s = scores[n] * HD ** -0.5 - slope * (length - pos).astype(F32)
            s = jnp.where(valid, s, NEG)
            top = jnp.max(s, axis=1, keepdims=True)
            p = jnp.where(valid, jnp.exp(s - top), 0.0)
            total = jnp.sum(p, axis=1, keepdims=True)
            weights.append(p.astype(BF16))
            stats = jnp.where(lane == j, top, jnp.where(lane == 64 + j, total, stats))
        for n in range(CP):
            j = i * CP + n
            v2 = jnp.concatenate([v_buf[0, j], v_buf[1, j]], axis=1)
            o = jnp.dot(weights[n], v2, preferred_element_type=F32)
            for c in range(2):
                piece = jnp.where(second_o, o[c * 8:(c + 1) * 8, HD:], o[c * 8:(c + 1) * 8, :HD])
                o_ref[c, i // (CH // 2), pl.ds(pl.multiple_of((j % 16) * 8, 8), 8), :] = piece
        for c in kv_out(i):
            c.start()
        return stats

    stats = lax.fori_loop(0, CH, chunk, jnp.zeros((16, HD), F32))
    for c in range(2):
        for x in range(2):
            o_ref[c, x, 128:136, :] = stats[c * 8:(c + 1) * 8]
    for i in range(CH):
        for c in kv_out(i):
            c.wait()


def rest_kernel(o_ref, x_hbm, g_hbm, wo_hbm, wu_hbm, wd_hbm, out_ref,
                x_buf, g_buf, wo_buf, wu_buf, wd_buf, o_recv, att, a_send, a_recv, y_send, y_recv, r_buf,
                hid, d_send, d_recv, z_send, z_recv, f_send, f_recv,
                in_sem, wo_sem, wu_sem, wd_sem, o_ss, o_rs, a_ss, a_rs, y_ss, y_rs, r_ss, r_rs,
                d_ss, d_rs, z_ss, z_rs, f_ss, f_rs):
    sp = lax.axis_index("sp")
    tp = lax.axis_index("tp")
    x = sp // 2
    c = sp % 2
    core = {"sp": x * 2 + (1 - c)}
    flip = {"sp": (1 - x) * 2 + c}
    other_tp = {"tp": 1 - tp}
    half = D // 2
    w = half // NOC

    def remote(src, dst, ss, rs, dev):
        return pltpu.make_async_remote_copy(src_ref=src, dst_ref=dst, send_sem=ss, recv_sem=rs, device_id=dev,
                                            device_id_type=MESH)

    wo_copy, wd_copy = [], []
    for n in range(2):
        cols = pl.ds(pl.multiple_of(((1 - c) if n == 0 else c) * half, half), half)
        wo_copy.append(pltpu.make_async_copy(wo_hbm.at[pl.ds(pl.multiple_of(c * 512, 512), 512), cols], wo_buf.at[n],
                                             wo_sem.at[n]))
        for k in range(NOC):
            cols = pl.ds(pl.multiple_of(((1 - c) if n == 0 else c) * half + k * w, w), w)
            wd_copy.append(pltpu.make_async_copy(wd_hbm.at[pl.ds(pl.multiple_of(c * FH, FH), FH), cols],
                                                 wd_buf.at[n * NOC + k], wd_sem.at[n * NOC + k]))
    wu_copy = [pltpu.make_async_copy(wu_hbm.at[:, pl.ds(pl.multiple_of(c * FH + k * (FH // NUP), FH // NUP), FH // NUP)],
                                     wu_buf.at[k], wu_sem.at[k]) for k in range(NUP)]
    in_copy = [pltpu.make_async_copy(g_hbm, g_buf, in_sem.at[0])]
    for n in range(2):
        in_copy.append(pltpu.make_async_copy(
            x_hbm.at[pl.ds(pl.multiple_of(n * 32 + x * 16, 16), 16), pl.ds(pl.multiple_of(c * half, half), half)],
            x_buf.at[n], in_sem.at[1 + n]))
    for cp in wo_copy + in_copy + wu_copy + wd_copy:
        cp.start()

    barrier = pltpu.get_barrier_semaphore()
    for rel in range(1, 4):
        pl.semaphore_signal(barrier, inc=1, device_id={"sp": (sp + rel) % 4}, device_id_type=MESH)
    pl.semaphore_signal(barrier, inc=1, device_id=other_tp, device_id_type=MESH)
    pl.semaphore_wait(barrier, 4)

    o_copy = []
    for rel in range(1, 4):
        peer = (sp + rel) % 4
        o_copy.append(remote(o_ref.at[peer % 2, peer // 2], o_recv.at[rel - 1], o_ss.at[rel - 1], o_rs.at[rel - 1],
                             {"sp": peer}))
    for cp in o_copy:
        cp.start()
    for cp in o_copy:
        cp.wait()
    parts = [o_ref.at[c, x]] + [o_recv.at[n] for n in range(3)]
    shift = (HD - 16 * x) % HD
    tops = [pltpu.roll(p[128:136, :], shift, 1) for p in parts]
    sums = [pltpu.roll(t, 64, 1) for t in tops]
    top = functools.reduce(jnp.maximum, tops)
    scale = [jnp.exp(t - top) for t in tops]
    total = functools.reduce(jnp.add, [a * s for a, s in zip(scale, sums)])
    scale = [a / total for a in scale]
    for j in range(16):
        acc = None
        for a, p in zip(scale, parts):
            term = p[j * 8:(j + 1) * 8, :] * a[:, j:j + 1]
            acc = term if acc is None else acc + term
        att[j * 8:(j + 1) * 8, :] = acc

    rows = []
    for bb in range(2):
        rows.append(jnp.concatenate([att[pl.ds(bb * 4 + h, 16, stride=8), :] for h in range(4)], axis=1))
    attended = jnp.concatenate(rows, axis=0).astype(BF16)
    wo_copy[0].wait()
    a_copy = []
    for k in range(NOC):
        a_send[k] = jnp.dot(attended, wo_buf[0, :, k * w:(k + 1) * w], preferred_element_type=F32)
        a_copy.append(remote(a_send.at[k], a_recv.at[k], a_ss.at[k], a_rs.at[k], core))
        a_copy[k].start()
    wo_copy[1].wait()
    own = [jnp.dot(attended, wo_buf[1, :, k * w:(k + 1) * w], preferred_element_type=F32) for k in range(NOC)]
    y_copy = []
    for k in range(NOC):
        a_copy[k].wait()
        y_send[k] = own[k] + a_recv[k]
        y_copy.append(remote(y_send.at[k], y_recv.at[k], y_ss.at[k], y_rs.at[k], other_tp))
        y_copy[k].start()
    for cp in in_copy:
        cp.wait()
    x_in = jnp.concatenate([x_buf[0], x_buf[1]], axis=0).astype(F32)
    r_copy = []
    for k in range(NOC):
        y_copy[k].wait()
        r_buf[c, k] = x_in[:, k * w:(k + 1) * w] + (y_send[k] + y_recv[k])
        r_copy.append(remote(r_buf.at[c, k], r_buf.at[c, k], r_ss.at[k], r_rs.at[k], core))
        r_copy[k].start()
    for cp in r_copy:
        cp.wait()

    res = jnp.concatenate([r_buf[n, k] for n in range(2) for k in range(NOC)], axis=1)
    normed = layer_norm(res, g_buf[...]).astype(BF16)
    fw = FH // NUP
    for k in range(NUP):
        wu_copy[k].wait()
        u = jnp.dot(normed, wu_buf[k], preferred_element_type=F32)
        hid[:, k * fw:(k + 1) * fw] = (0.5 * u * (1.0 + lax.erf(u * 0.5 ** 0.5))).astype(BF16)
    d_copy = []
    for k in range(NOC):
        wd_copy[k].wait()
        d_send[k] = jnp.dot(hid[...], wd_buf[k], preferred_element_type=F32)
        d_copy.append(remote(d_send.at[k], d_recv.at[k], d_ss.at[k], d_rs.at[k], core))
        d_copy[k].start()
    z_copy = []
    for k in range(NOC):
        wd_copy[NOC + k].wait()
        mine = jnp.dot(hid[...], wd_buf[NOC + k], preferred_element_type=F32)
        d_copy[k].wait()
        z_send[k] = mine + d_recv[k]
        z_copy.append(remote(z_send.at[k], z_recv.at[k], z_ss.at[k], z_rs.at[k], other_tp))
        z_copy[k].start()

    def put(block, where, cc, k):
        for n in range(2):
            out_ref[pl.ds(pl.multiple_of(n * 32 + where * 16, 16), 16),
                    pl.ds(pl.multiple_of(cc * half + k * w, w), w)] = block[n * 16:(n + 1) * 16].astype(BF16)

    near, far, fwd = [], [], []
    for k in range(NOC):
        z_copy[k].wait()
        val = r_buf[c, k] + (z_send[k] + z_recv[k])
        f_send[k] = val
        far.append(remote(f_send.at[k], f_recv.at[1, k], f_ss.at[1, k], f_rs.at[1, k], flip))
        far[k].start()
        near.append(remote(f_send.at[k], f_recv.at[0, k], f_ss.at[0, k], f_rs.at[0, k], core))
        near[k].start()
        put(val, x, c, k)
    for k in range(NOC):
        far[k].wait()
        fwd.append(remote(f_recv.at[1, k], f_recv.at[2, k], f_ss.at[2, k], f_rs.at[2, k], core))
        fwd[k].start()
        put(f_recv[1, k], 1 - x, c, k)
    for k in range(NOC):
        near[k].wait()
        put(f_recv[0, k], x, 1 - c, k)
    for k in range(NOC):
        fwd[k].wait()
        put(f_recv[2, k], 1 - x, 1 - c, k)


def solution(mesh):
    def hbm(a):
        return pltpu.with_memory_space_constraint(a, pltpu.HBM)

    in_hbm = pl.BlockSpec(memory_space=pltpu.HBM)
    in_vmem = pl.BlockSpec(memory_space=pltpu.VMEM)
    dma = pltpu.SemaphoreType.DMA

    def local_layer(x_in, seq_lens, k_cache, v_cache, ln1_gain, w_qkv, w_out, ln2_gain, w_up, w_down):
        caches = [hbm(a.reshape(2, B // 2, T * NH, HD)) for a in (k_cache, v_cache)]
        cache_type = jax.ShapeDtypeStruct((2, B // 2, T * NH, HD), BF16)
        w_split, lhs = pl.pallas_call(
            prepare_kernel,
            out_shape=[pltpu.VMEM((12, D, 2, HD), BF16), pltpu.VMEM((2 * B, NQ), BF16)],
            in_specs=[in_hbm] * 3,
            out_specs=[in_vmem, in_vmem],
            scratch_shapes=[pltpu.VMEM((B, D), BF16), pltpu.VMEM((1, D), F32), dma((2,)), dma((12,))],
            compiler_params=pltpu.CompilerParams(vmem_limit_bytes=16 * 1024 * 1024),
            name="prepare",
        )(hbm(x_in), hbm(ln1_gain.reshape(1, D)), hbm(w_qkv.reshape(D, 12, 2, HD)))
        k_next, v_next, parts = pl.pallas_call(
            attend_kernel,
            out_shape=[cache_type, cache_type, jax.ShapeDtypeStruct((2, 2, 136, HD), F32)],
            in_specs=[in_vmem] * 2 + [in_hbm] * 3,
            out_specs=[in_hbm, in_hbm, in_vmem],
            scratch_shapes=[
                pltpu.SMEM((B,), jnp.int32),
                pltpu.VMEM((2, B // 2, T * NH, HD), BF16), pltpu.VMEM((2, B // 2, T * NH, HD), BF16),
                pltpu.VMEM((B * NH, HD), F32), pltpu.VMEM((B * NH, HD), F32), pltpu.VMEM((B * NH, HD), F32),
                dma, dma((CH,)), dma((CH,)), dma((CH,)), dma((CH,)),
            ],
            compiler_params=pltpu.CompilerParams(vmem_limit_bytes=36 * 1024 * 1024),
            name="attend",
        )(lhs, w_split.reshape(12, NQ, HD), hbm(seq_lens), *caches)
        w = D // 2 // NOC
        x_out = pl.pallas_call(
            rest_kernel,
            out_shape=jax.ShapeDtypeStruct((B, D), BF16),
            in_specs=[in_vmem] + [in_hbm] * 5,
            out_specs=in_vmem,
            scratch_shapes=[
                pltpu.VMEM((2, 16, D // 2), BF16), pltpu.VMEM((1, D), F32),
                pltpu.VMEM((2, 512, D // 2), BF16), pltpu.VMEM((NUP, D, FH // NUP), BF16),
                pltpu.VMEM((2 * NOC, FH, w), BF16),
                pltpu.VMEM((3, 136, HD), F32), pltpu.VMEM((128, HD), F32),
                pltpu.VMEM((NOC, 32, w), F32), pltpu.VMEM((NOC, 32, w), F32),
                pltpu.VMEM((NOC, 32, w), F32), pltpu.VMEM((NOC, 32, w), F32),
                pltpu.VMEM((2, NOC, 32, w), F32),
                pltpu.VMEM((32, FH), BF16),
                pltpu.VMEM((NOC, 32, w), F32), pltpu.VMEM((NOC, 32, w), F32),
                pltpu.VMEM((NOC, 32, w), F32), pltpu.VMEM((NOC, 32, w), F32),
                pltpu.VMEM((NOC, 32, w), F32), pltpu.VMEM((3, NOC, 32, w), F32),
                dma((3,)), dma((2,)), dma((NUP,)), dma((2 * NOC,)), dma((3,)), dma((3,)),
                dma((NOC,)), dma((NOC,)), dma((NOC,)), dma((NOC,)), dma((NOC,)), dma((NOC,)),
                dma((NOC,)), dma((NOC,)), dma((NOC,)), dma((NOC,)), dma((3, NOC)), dma((3, NOC)),
            ],
            compiler_params=pltpu.CompilerParams(vmem_limit_bytes=32 * 1024 * 1024, collective_id=0,
                                                 has_side_effects=True),
            name="rest",
        )(parts, hbm(x_in), hbm(ln2_gain.reshape(1, D)), hbm(w_out.reshape(NH * HD, D)), hbm(w_up), hbm(w_down))
        return x_out, k_next.reshape(k_cache.shape), v_next.reshape(v_cache.shape)

    cache_spec = P("dp", "sp", "tp", None)
    in_specs = (P("dp", None), P("dp"), cache_spec, cache_spec, P(None), P(None, None, "tp", None), P("tp", None, None), P(None), P(None, "tp"), P("tp", None))
    out_specs = (P("dp", None), cache_spec, cache_spec)
    return jax.shard_map(local_layer, mesh=mesh, in_specs=in_specs, out_specs=out_specs, check_vma=False)
```

```python
import functools

import jax
import jax.numpy as jnp
from jax import lax
from jax.experimental import pallas as pl
from jax.experimental.pallas import tpu as pltpu
from jax.sharding import PartitionSpec as P

LN_EPS = 1e-5
NEG = -1e30
F32 = jnp.float32
BF16 = jnp.bfloat16
MESH = pl.DeviceIdType.MESH

B = 64
D = 2048
NH = 8
HD = 128
T = 64
NQ = 2 * D
CH = 4
CP = 32 // CH
FH = 2048
AHEAD = 4
NUP = 4
NY = 4
NZ = 4


def layer_norm(x_f32, gain):
    mean = jnp.mean(x_f32, axis=-1, keepdims=True)
    centred = x_f32 - mean
    variance = jnp.mean(centred * centred, axis=-1, keepdims=True)
    return centred * lax.rsqrt(variance + LN_EPS) * gain


def prepare_kernel(x_hbm, g_hbm, w_hbm, w_out, lhs, x_buf, g_buf, small_sem, w_sem):
    small = [pltpu.make_async_copy(x_hbm, x_buf, small_sem.at[0]),
             pltpu.make_async_copy(g_hbm, g_buf, small_sem.at[1])]
    w_copy = [pltpu.make_async_copy(w_hbm.at[:, i], w_out.at[i], w_sem.at[i]) for i in range(12)]
    for c in small + w_copy:
        c.start()
    for c in small:
        c.wait()
    normed = layer_norm(x_buf[...].astype(F32), g_buf[...]).astype(BF16)
    spread = (lax.broadcasted_iota(jnp.int32, (128, 256), 1) // 2
              == lax.broadcasted_iota(jnp.int32, (128, 256), 0)).astype(BF16)
    odd = lax.broadcasted_iota(jnp.int32, (B, 256), 1) % 2 == 1
    for i in range(D // 128):
        twice = jnp.dot(normed[:, i * 128:(i + 1) * 128], spread, preferred_element_type=F32)
        lhs[0:B, i * 256:(i + 1) * 256] = jnp.where(odd, 0.0, twice).astype(BF16)
        lhs[B:2 * B, i * 256:(i + 1) * 256] = jnp.where(odd, twice, 0.0).astype(BF16)
    for c in w_copy:
        c.wait()


def attend_kernel(lhs, w_ref, lens_hbm, k_hbm, v_hbm, k_buf, v_buf, o_ref,
                  lens, q_s, k_s, v_s, small_sem, kin_sem, vin_sem):
    lens_copy = pltpu.make_async_copy(lens_hbm, lens, small_sem)
    lens_copy.start()

    def kv_in(i):
        at = pl.ds(i * 2 * CP, 2 * CP)
        return (pltpu.make_async_copy(k_hbm.at[at], k_buf.at[at], kin_sem.at[i]),
                pltpu.make_async_copy(v_hbm.at[at], v_buf.at[at], vin_sem.at[i]))

    for i in range(AHEAD):
        for c in kv_in(i):
            c.start()

    for i in range(0, 12, 2):
        two = jnp.concatenate([w_ref[i], w_ref[i + 1]], axis=1)
        res = jnp.dot(lhs[...], two, preferred_element_type=F32)
        for n in range(2):
            part, pair = divmod(i + n, 4)
            for parity in range(2):
                h = 2 * pair + parity
                val = res[parity * B:(parity + 1) * B, n * HD:(n + 1) * HD]
                (q_s, k_s, v_s)[part][pl.ds(h, B, stride=NH), :] = val
    lens_copy.wait()

    sp = lax.axis_index("sp")
    tp = lax.axis_index("tp")
    row = lax.broadcasted_iota(jnp.int32, (16, 1), 0)
    slope = jnp.exp2(-8.0 * (tp * NH + row % NH + 1).astype(F32) / (2 * NH))
    col = lax.broadcasted_iota(jnp.int32, (16, NH * T), 1)
    own_head = col % NH == lax.broadcasted_iota(jnp.int32, (16, NH * T), 0) % NH
    pos = jnp.where(own_head, sp * T + col // NH, 1 << 20)
    second = row >= 8
    upper = lax.broadcasted_iota(jnp.int32, (16, HD), 0) >= 8
    lane = lax.broadcasted_iota(jnp.int32, (16, HD), 1)

    def insert(buf, new, b):
        slot = lens[b] - sp * T
        held = jnp.logical_and(slot >= 0, slot < T)
        at = jnp.clip(slot, 0, T - 1)
        rows = pl.ds(pl.multiple_of((at // 2) * 16, 16), 16)
        fresh = new[pl.ds(pl.multiple_of(b * NH, NH), NH), :]
        fresh = jnp.concatenate([fresh, fresh], axis=0)
        keep = jnp.where(held, at % 2, 2)
        old = buf[b, rows, :].astype(F32)
        buf[b, rows, :] = jnp.where(upper.astype(jnp.int32) == keep, fresh, old).astype(BF16)

    def chunk(step, stats):
        for c in kv_in(step):
            c.wait()

        @pl.when(step + AHEAD < CH)
        def _():
            for c in kv_in(step + AHEAD):
                c.start()

        for n in range(2 * CP):
            insert(k_buf, k_s, step * 2 * CP + n)
            insert(v_buf, v_s, step * 2 * CP + n)
        scores = []
        for n in range(CP):
            j = step * CP + n
            q = q_s[pl.ds(pl.multiple_of(j * 16, 16), 16), :]
            q2 = jnp.concatenate([jnp.where(upper, 0.0, q), jnp.where(upper, q, 0.0)], axis=1).astype(BF16)
            k2 = jnp.concatenate([k_buf[2 * j], k_buf[2 * j + 1]], axis=1)
            scores.append(lax.dot_general(q2, k2, (((1,), (1,)), ((), ())), preferred_element_type=F32))
        weights = []
        for n in range(CP):
            j = step * CP + n
            length = jnp.where(second, lens[2 * j + 1], lens[2 * j])
            valid = pos <= length
            s = scores[n] * HD ** -0.5 - slope * (length - pos).astype(F32)
            s = jnp.where(valid, s, NEG)
            top = jnp.max(s, axis=1, keepdims=True)
            p = jnp.where(valid, jnp.exp(s - top), 0.0)
            total = jnp.sum(p, axis=1, keepdims=True)
            weights.append(p.astype(BF16))
            stats = jnp.where(lane == j, top, jnp.where(lane == 64 + j, total, stats))
        for n in range(CP):
            j = step * CP + n
            v2 = jnp.concatenate([v_buf[2 * j], v_buf[2 * j + 1]], axis=1)
            o = jnp.dot(weights[n], v2, preferred_element_type=F32)
            at = pl.multiple_of((j % 8) * 16, 16)
            o_ref[j // 8, pl.ds(at, 8), :] = o[0:8, :HD]
            o_ref[j // 8, pl.ds(at + 8, 8), :] = o[8:16, HD:]
        return stats

    stats = lax.fori_loop(0, CH, chunk, jnp.zeros((16, HD), F32))
    for i in range(4):
        o_ref[i, 128:144, :] = stats


def write_kernel(k_buf, v_buf, ko_hbm, vo_hbm, k_sem, v_sem):
    copies = []
    for i in range(4):
        at = pl.ds(i * (B // 4), B // 4)
        copies.append(pltpu.make_async_copy(k_buf.at[at], ko_hbm.at[at], k_sem.at[i]))
        copies.append(pltpu.make_async_copy(v_buf.at[at], vo_hbm.at[at], v_sem.at[i]))
    for c in copies:
        c.start()
    for c in copies:
        c.wait()


def rest_kernel(o0, o1, o2, o3, wo_ref, x_hbm, g_hbm, wu_hbm, wd_hbm, out_ref,
                x_buf, g_buf, wu_buf, wd_buf, att, y_send, y_recv, r_buf, r_recv, n_send, n_recv,
                hid, h_send, h_recv, z_send, z_recv, f_send, f_recv,
                in_sem, wu_sem, wd_sem, y_ss, y_rs, r_ss, r_rs, n_ss, n_rs, h_ss, h_rs, z_ss, z_rs, f_ss, f_rs):
    sp = lax.axis_index("sp")
    tp = lax.axis_index("tp")
    x = sp // 2
    c = sp % 2
    core = {"sp": x * 2 + (1 - c)}
    flip = {"sp": (1 - x) * 2 + c}
    other_tp = {"tp": 1 - tp}
    half = D // 2
    yw = D // NY
    fw = FH // NUP
    zw = half // NZ

    def remote(src, dst, ss, rs, dev):
        return pltpu.make_async_remote_copy(src_ref=src, dst_ref=dst, send_sem=ss, recv_sem=rs, device_id=dev,
                                            device_id_type=MESH)

    barrier = pltpu.get_barrier_semaphore()
    for dev in (core, flip, other_tp):
        pl.semaphore_signal(barrier, inc=1, device_id=dev, device_id_type=MESH)

    in_copy = [pltpu.make_async_copy(g_hbm, g_buf, in_sem.at[0]),
               pltpu.make_async_copy(x_hbm.at[pl.ds(pl.multiple_of(sp * 16, 16), 16)], x_buf, in_sem.at[1])]
    wu_copy = [pltpu.make_async_copy(wu_hbm.at[:, pl.ds(pl.multiple_of(c * FH + k * fw, fw), fw)],
                                     wu_buf.at[k], wu_sem.at[k]) for k in range(NUP)]
    wd_copy = [pltpu.make_async_copy(wd_hbm.at[pl.ds(pl.multiple_of((c if n == 0 else 1 - c) * FH, FH), FH),
                                               pl.ds(pl.multiple_of(c * half, half), half)],
                                     wd_buf.at[n], wd_sem.at[n]) for n in range(2)]
    for cp in in_copy + wu_copy:
        cp.start()

    parts = [o0, o1, o2, o3]
    shift = lax.rem(HD - 8 * sp, HD)
    tops = [pltpu.roll(p[128:144, :], shift, 1) for p in parts]
    sums = [pltpu.roll(t, 64, 1) for t in tops]
    top = functools.reduce(jnp.maximum, tops)
    scale = [jnp.exp(t - top) for t in tops]
    total = functools.reduce(jnp.add, [a * s for a, s in zip(scale, sums)])
    scale = [a / total for a in scale]
    for j in range(8):
        acc = None
        for a, p in zip(scale, parts):
            term = p[j * 16:(j + 1) * 16, :] * a[:, j:j + 1]
            acc = term if acc is None else acc + term
        att[j * 16:(j + 1) * 16, :] = acc
    attended = jnp.concatenate([att[pl.ds(h, 16, stride=NH), :] for h in range(NH)], axis=1).astype(BF16)

    pl.semaphore_wait(barrier, 3)
    y_copy = []
    for k in range(NY):
        y_send[k] = jnp.dot(attended, wo_ref[:, k * yw:(k + 1) * yw], preferred_element_type=F32)
        y_copy.append(remote(y_send.at[k], y_recv.at[k], y_ss.at[k], y_rs.at[k], other_tp))
        y_copy[k].start()
    for cp in wd_copy:
        cp.start()
    for cp in in_copy:
        cp.wait()
    for k in range(NY):
        y_copy[k].wait()
        r_buf[k // (NY // 2), :, (k % (NY // 2)) * yw:(k % (NY // 2) + 1) * yw] = \
            x_buf[:, k * yw:(k + 1) * yw].astype(F32) + (y_send[k] + y_recv[k])
    normed = layer_norm(jnp.concatenate([r_buf[0], r_buf[1]], axis=1), g_buf[...]).astype(BF16)
    n_send[...] = normed.astype(F32)
    n_copy = remote(n_send, n_recv, n_ss, n_rs, core)
    n_copy.start()
    r_copy = remote(r_buf.at[1 - c], r_recv, r_ss, r_rs, core)
    r_copy.start()
    n_copy.wait()
    both = jnp.concatenate([normed, n_recv[...].astype(BF16)], axis=0)

    h_copy = []
    for k in range(NUP):
        wu_copy[k].wait()
        u = jnp.dot(both, wu_buf[k], preferred_element_type=F32)
        act = (0.5 * u * (1.0 + lax.erf(u * 0.5 ** 0.5))).astype(BF16)
        hid[:, k * fw:(k + 1) * fw] = act
        h_send[k] = act.astype(F32)
        h_copy.append(remote(h_send.at[k], h_recv.at[k], h_ss.at[k], h_rs.at[k], core))
        h_copy[k].start()
    wd_copy[0].wait()
    mine = [jnp.dot(hid[...], wd_buf[0, :, k * zw:(k + 1) * zw], preferred_element_type=F32) for k in range(NZ)]
    wd_copy[1].wait()
    theirs = []
    for k in range(NUP):
        h_copy[k].wait()
        theirs.append(jnp.concatenate([h_recv[k, 16:32, :], h_recv[k, 0:16, :]], axis=0).astype(BF16))
    theirs = jnp.concatenate(theirs, axis=1)
    z_copy = []
    for k in range(NZ):
        z_send[k] = mine[k] + jnp.dot(theirs, wd_buf[1, :, k * zw:(k + 1) * zw], preferred_element_type=F32)
        z_copy.append(remote(z_send.at[k], z_recv.at[k], z_ss.at[k], z_rs.at[k], other_tp))
        z_copy[k].start()

    def put(block, first, second, cc, k):
        for n, where in enumerate((first, second)):
            out_ref[pl.ds(pl.multiple_of(where * 16, 16), 16),
                    pl.ds(pl.multiple_of(cc * half + k * zw, zw), zw)] = block[n * 16:(n + 1) * 16].astype(BF16)

    sp_core = x * 2 + (1 - c)
    sp_flip = (1 - x) * 2 + c
    sp_diag = (1 - x) * 2 + (1 - c)
    r_copy.wait()
    near, far, fwd = [], [], []
    for k in range(NZ):
        z_copy[k].wait()
        res = jnp.concatenate([r_buf[c, :, k * zw:(k + 1) * zw], r_recv[:, k * zw:(k + 1) * zw]], axis=0)
        val = res + (z_send[k] + z_recv[k])
        f_send[k] = val
        far.append(remote(f_send.at[k], f_recv.at[1, k], f_ss.at[1, k], f_rs.at[1, k], flip))
        far[k].start()
        near.append(remote(f_send.at[k], f_recv.at[0, k], f_ss.at[0, k], f_rs.at[0, k], core))
        near[k].start()
        put(val, sp, sp_core, c, k)
    for k in range(NZ):
        far[k].wait()
        fwd.append(remote(f_recv.at[1, k], f_recv.at[2, k], f_ss.at[2, k], f_rs.at[2, k], core))
        fwd[k].start()
        put(f_recv[1, k], sp_flip, sp_diag, c, k)
        near[k].wait()
        put(f_recv[0, k], sp_core, sp, 1 - c, k)
    for k in range(NZ):
        fwd[k].wait()
        put(f_recv[2, k], sp_diag, sp_flip, 1 - c, k)


def solution(mesh):
    def hbm(a):
        return pltpu.with_memory_space_constraint(a, pltpu.HBM)

    in_hbm = pl.BlockSpec(memory_space=pltpu.HBM)
    in_vmem = pl.BlockSpec(memory_space=pltpu.VMEM)
    dma = pltpu.SemaphoreType.DMA

    def local_layer(x_in, seq_lens, k_cache, v_cache, ln1_gain, w_qkv, w_out, ln2_gain, w_up, w_down):
        caches = [hbm(a.reshape(B, T * NH, HD)) for a in (k_cache, v_cache)]
        sp = lax.axis_index("sp")
        w_split, lhs = pl.pallas_call(
            prepare_kernel,
            out_shape=[pltpu.VMEM((12, D, 2, HD), BF16), pltpu.VMEM((2 * B, NQ), BF16)],
            in_specs=[in_hbm] * 3,
            out_specs=[in_vmem, in_vmem],
            scratch_shapes=[pltpu.VMEM((B, D), BF16), pltpu.VMEM((1, D), F32), dma((2,)), dma((12,))],
            compiler_params=pltpu.CompilerParams(vmem_limit_bytes=16 * 1024 * 1024),
            name="prepare",
        )(hbm(x_in), hbm(ln1_gain.reshape(1, D)), hbm(w_qkv.reshape(D, 12, 2, HD)))
        cache_shape = (B, T * NH, HD)
        k_upd, v_upd, parts = pl.pallas_call(
            attend_kernel,
            out_shape=[pltpu.VMEM(cache_shape, BF16), pltpu.VMEM(cache_shape, BF16),
                       jax.ShapeDtypeStruct((4, 144, HD), F32)],
            in_specs=[in_vmem] * 2 + [in_hbm] * 3,
            out_specs=[in_vmem] * 3,
            scratch_shapes=[
                pltpu.SMEM((B,), jnp.int32),
                pltpu.VMEM((B * NH, HD), F32), pltpu.VMEM((B * NH, HD), F32), pltpu.VMEM((B * NH, HD), F32),
                dma, dma((CH,)), dma((CH,)),
            ],
            compiler_params=pltpu.CompilerParams(vmem_limit_bytes=8 * 1024 * 1024),
            name="attend",
        )(lhs, w_split.reshape(12, NQ, HD), hbm(seq_lens), *caches)
        pieces = [lax.dynamic_index_in_dim(parts, (sp + rel) % 4, 0, keepdims=False) for rel in range(4)]
        moved = [lax.ppermute(pieces[rel], "sp", [(i, (i + rel) % 4) for i in range(4)]) for rel in (1, 2, 3)]
        k_next, v_next = pl.pallas_call(
            write_kernel,
            out_shape=[jax.ShapeDtypeStruct(cache_shape, BF16)] * 2,
            in_specs=[in_vmem] * 2,
            out_specs=[in_hbm] * 2,
            scratch_shapes=[dma((4,)), dma((4,))],
            compiler_params=pltpu.CompilerParams(vmem_limit_bytes=8 * 1024 * 1024),
            cost_estimate=pl.CostEstimate(flops=6 * 10 ** 9, bytes_accessed=16 << 20, transcendentals=0),
            name="write",
        )(k_upd, v_upd)
        x_out = pl.pallas_call(
            rest_kernel,
            out_shape=jax.ShapeDtypeStruct((B, D), BF16),
            in_specs=[in_vmem] * 5 + [in_hbm] * 4,
            out_specs=in_vmem,
            scratch_shapes=[
                pltpu.VMEM((16, D), BF16), pltpu.VMEM((1, D), F32),
                pltpu.VMEM((NUP, D, FH // NUP), BF16),
                pltpu.VMEM((2, FH, D // 2), BF16),
                pltpu.VMEM((128, HD), F32),
                pltpu.VMEM((NY, 16, D // NY), F32), pltpu.VMEM((NY, 16, D // NY), F32),
                pltpu.VMEM((2, 16, D // 2), F32), pltpu.VMEM((16, D // 2), F32),
                pltpu.VMEM((16, D), F32), pltpu.VMEM((16, D), F32),
                pltpu.VMEM((32, FH), BF16),
                pltpu.VMEM((NUP, 32, FH // NUP), F32), pltpu.VMEM((NUP, 32, FH // NUP), F32),
                pltpu.VMEM((NZ, 32, D // 2 // NZ), F32), pltpu.VMEM((NZ, 32, D // 2 // NZ), F32),
                pltpu.VMEM((NZ, 32, D // 2 // NZ), F32), pltpu.VMEM((3, NZ, 32, D // 2 // NZ), F32),
                dma((2,)), dma((NUP,)), dma((2,)),
                dma((NY,)), dma((NY,)), dma, dma, dma, dma, dma((NUP,)), dma((NUP,)),
                dma((NZ,)), dma((NZ,)), dma((3, NZ)), dma((3, NZ)),
            ],
            compiler_params=pltpu.CompilerParams(vmem_limit_bytes=32 * 1024 * 1024, collective_id=0,
                                                 has_side_effects=True),
            cost_estimate=pl.CostEstimate(flops=10 ** 10, bytes_accessed=20 << 20, transcendentals=0),
            name="rest",
        )(pieces[0], *moved, w_out.reshape(NH * HD, D), hbm(x_in), hbm(ln2_gain.reshape(1, D)), hbm(w_up), hbm(w_down))
        return x_out, k_next.reshape(k_cache.shape), v_next.reshape(v_cache.shape)

    cache_spec = P("dp", "sp", "tp", None)
    in_specs = (P("dp", None), P("dp"), cache_spec, cache_spec, P(None), P(None, None, "tp", None), P("tp", None, None), P(None), P(None, "tp"), P("tp", None))
    out_specs = (P("dp", None), cache_spec, cache_spec)
    return jax.shard_map(local_layer, mesh=mesh, in_specs=in_specs, out_specs=out_specs, check_vma=False)
```

```python
import functools

import jax
import jax.numpy as jnp
from jax import lax
from jax.experimental import pallas as pl
from jax.experimental.pallas import tpu as pltpu
from jax.sharding import PartitionSpec as P

LN_EPS = 1e-5
NEG = -1e30
F32 = jnp.float32
BF16 = jnp.bfloat16
MESH = pl.DeviceIdType.MESH

B = 64
D = 2048
NH = 8
HD = 128
T = 64
NQ = 2 * D
CH = 4
CP = 32 // CH
AHEAD = 4
NUP = 2
NY = 4
NZ = 4


def layer_norm(x_f32, gain):
    mean = jnp.mean(x_f32, axis=-1, keepdims=True)
    centred = x_f32 - mean
    variance = jnp.mean(centred * centred, axis=-1, keepdims=True)
    return centred * lax.rsqrt(variance + LN_EPS) * gain


def prepare_kernel(x_hbm, g_hbm, w_hbm, w_out, lhs, x_buf, g_buf, small_sem, w_sem):
    small = [pltpu.make_async_copy(x_hbm, x_buf, small_sem.at[0]),
             pltpu.make_async_copy(g_hbm, g_buf, small_sem.at[1])]
    w_copy = [pltpu.make_async_copy(w_hbm.at[:, i], w_out.at[i], w_sem.at[i]) for i in range(12)]
    for c in small + w_copy:
        c.start()
    for c in small:
        c.wait()
    normed = layer_norm(x_buf[...].astype(F32), g_buf[...]).astype(BF16)
    spread = (lax.broadcasted_iota(jnp.int32, (128, 256), 1) // 2
              == lax.broadcasted_iota(jnp.int32, (128, 256), 0)).astype(BF16)
    odd = lax.broadcasted_iota(jnp.int32, (B, 256), 1) % 2 == 1
    for i in range(D // 128):
        twice = jnp.dot(normed[:, i * 128:(i + 1) * 128], spread, preferred_element_type=F32)
        lhs[0:B, i * 256:(i + 1) * 256] = jnp.where(odd, 0.0, twice).astype(BF16)
        lhs[B:2 * B, i * 256:(i + 1) * 256] = jnp.where(odd, twice, 0.0).astype(BF16)
    for c in w_copy:
        c.wait()


def attend_kernel(lhs, w_ref, lens_hbm, k_hbm, v_hbm, k_buf, v_buf, o_ref,
                  lens, q_s, k_s, v_s, small_sem, kin_sem, vin_sem):
    lens_copy = pltpu.make_async_copy(lens_hbm, lens, small_sem)
    lens_copy.start()

    def kv_in(i):
        at = pl.ds(i * 2 * CP, 2 * CP)
        return (pltpu.make_async_copy(k_hbm.at[at], k_buf.at[at], kin_sem.at[i]),
                pltpu.make_async_copy(v_hbm.at[at], v_buf.at[at], vin_sem.at[i]))

    for i in range(AHEAD):
        for c in kv_in(i):
            c.start()

    for i in range(0, 12, 2):
        two = jnp.concatenate([w_ref[i], w_ref[i + 1]], axis=1)
        res = jnp.dot(lhs[...], two, preferred_element_type=F32)
        for n in range(2):
            part, pair = divmod(i + n, 4)
            for parity in range(2):
                h = 2 * pair + parity
                val = res[parity * B:(parity + 1) * B, n * HD:(n + 1) * HD]
                (q_s, k_s, v_s)[part][pl.ds(h, B, stride=NH), :] = val
    lens_copy.wait()

    sp = lax.axis_index("sp")
    tp = lax.axis_index("tp")
    row = lax.broadcasted_iota(jnp.int32, (16, 1), 0)
    slope = jnp.exp2(-8.0 * (tp * NH + row % NH + 1).astype(F32) / (2 * NH))
    col = lax.broadcasted_iota(jnp.int32, (16, NH * T), 1)
    own_head = col % NH == lax.broadcasted_iota(jnp.int32, (16, NH * T), 0) % NH
    pos = jnp.where(own_head, sp * T + col // NH, 1 << 20)
    second = row >= 8
    upper = lax.broadcasted_iota(jnp.int32, (16, HD), 0) >= 8
    lane = lax.broadcasted_iota(jnp.int32, (16, HD), 1)

    def insert(buf, new, b):
        slot = lens[b] - sp * T
        held = jnp.logical_and(slot >= 0, slot < T)
        at = jnp.clip(slot, 0, T - 1)
        rows = pl.ds(pl.multiple_of((at // 2) * 16, 16), 16)
        fresh = new[pl.ds(pl.multiple_of(b * NH, NH), NH), :]
        fresh = jnp.concatenate([fresh, fresh], axis=0)
        keep = jnp.where(held, at % 2, 2)
        old = buf[b, rows, :].astype(F32)
        buf[b, rows, :] = jnp.where(upper.astype(jnp.int32) == keep, fresh, old).astype(BF16)

    def chunk(step, stats):
        for c in kv_in(step):
            c.wait()

        @pl.when(step + AHEAD < CH)
        def _():
            for c in kv_in(step + AHEAD):
                c.start()

        for n in range(2 * CP):
            insert(k_buf, k_s, step * 2 * CP + n)
            insert(v_buf, v_s, step * 2 * CP + n)
        scores = []
        for n in range(CP):
            j = step * CP + n
            q = q_s[pl.ds(pl.multiple_of(j * 16, 16), 16), :]
            q2 = jnp.concatenate([jnp.where(upper, 0.0, q), jnp.where(upper, q, 0.0)], axis=1).astype(BF16)
            k2 = jnp.concatenate([k_buf[2 * j], k_buf[2 * j + 1]], axis=1)
            scores.append(lax.dot_general(q2, k2, (((1,), (1,)), ((), ())), preferred_element_type=F32))
        weights = []
        for n in range(CP):
            j = step * CP + n
            length = jnp.where(second, lens[2 * j + 1], lens[2 * j])
            valid = pos <= length
            s = scores[n] * HD ** -0.5 - slope * (length - pos).astype(F32)
            s = jnp.where(valid, s, NEG)
            top = jnp.max(s, axis=1, keepdims=True)
            p = jnp.where(valid, jnp.exp(s - top), 0.0)
            total = jnp.sum(p, axis=1, keepdims=True)
            weights.append(p.astype(BF16))
            stats = jnp.where(lane == j, top, jnp.where(lane == 64 + j, total, stats))
        for n in range(CP):
            j = step * CP + n
            v2 = jnp.concatenate([v_buf[2 * j], v_buf[2 * j + 1]], axis=1)
            o = jnp.dot(weights[n], v2, preferred_element_type=F32)
            at = pl.multiple_of((j % 8) * 16, 16)
            o_ref[j // 8, pl.ds(at, 8), :] = o[0:8, :HD]
            o_ref[j // 8, pl.ds(at + 8, 8), :] = o[8:16, HD:]
        return stats

    stats = lax.fori_loop(0, CH, chunk, jnp.zeros((16, HD), F32))
    for i in range(4):
        o_ref[i, 128:144, :] = stats


def write_kernel(k_buf, v_buf, ko_hbm, vo_hbm, k_sem, v_sem):
    copies = []
    for i in range(4):
        at = pl.ds(i * (B // 4), B // 4)
        copies.append(pltpu.make_async_copy(k_buf.at[at], ko_hbm.at[at], k_sem.at[i]))
        copies.append(pltpu.make_async_copy(v_buf.at[at], vo_hbm.at[at], v_sem.at[i]))
    for c in copies:
        c.start()
    for c in copies:
        c.wait()


def rest_kernel(o0, o1, o2, o3, wo_ref, x_hbm, g_hbm, wu_hbm, wd_hbm, out_ref,
                x_buf, g_buf, wu_buf, wd_buf, att, y_send, y_recv, r_buf, hid, z_send, z_recv, f_send, f_recv,
                in_sem, wu_sem, wd_sem, y_ss, y_rs, z_ss, z_rs, f_ss, f_rs):
    sp = lax.axis_index("sp")
    tp = lax.axis_index("tp")
    x = sp // 2
    c = sp % 2
    sp_core = x * 2 + (1 - c)
    sp_flip = (1 - x) * 2 + c
    sp_diag = (1 - x) * 2 + (1 - c)
    other_tp = {"tp": 1 - tp}
    yw = D // NY
    fw = wu_hbm.shape[1] // NUP
    zw = D // NZ

    def remote(src, dst, ss, rs, dev):
        return pltpu.make_async_remote_copy(src_ref=src, dst_ref=dst, send_sem=ss, recv_sem=rs, device_id=dev,
                                            device_id_type=MESH)

    barrier = pltpu.get_barrier_semaphore()
    for dev in ({"sp": sp_core}, {"sp": sp_flip}, {"sp": sp_diag}, other_tp):
        pl.semaphore_signal(barrier, inc=1, device_id=dev, device_id_type=MESH)

    in_copy = [pltpu.make_async_copy(g_hbm, g_buf, in_sem.at[0]),
               pltpu.make_async_copy(x_hbm.at[pl.ds(pl.multiple_of(sp * 16, 16), 16)], x_buf, in_sem.at[1])]
    wu_copy = [pltpu.make_async_copy(wu_hbm.at[:, k * fw:(k + 1) * fw], wu_buf.at[k], wu_sem.at[k]) for k in range(NUP)]
    wd_copy = [pltpu.make_async_copy(wd_hbm.at[:, k * zw:(k + 1) * zw], wd_buf.at[k], wd_sem.at[k]) for k in range(NZ)]
    for cp in in_copy + wu_copy:
        cp.start()

    parts = [o0, o1, o2, o3]
    shift = lax.rem(HD - 8 * sp, HD)
    tops = [pltpu.roll(p[128:144, :], shift, 1) for p in parts]
    sums = [pltpu.roll(t, 64, 1) for t in tops]
    top = functools.reduce(jnp.maximum, tops)
    scale = [jnp.exp(t - top) for t in tops]
    total = functools.reduce(jnp.add, [a * s for a, s in zip(scale, sums)])
    scale = [a / total for a in scale]
    for j in range(8):
        acc = None
        for a, p in zip(scale, parts):
            term = p[j * 16:(j + 1) * 16, :] * a[:, j:j + 1]
            acc = term if acc is None else acc + term
        att[j * 16:(j + 1) * 16, :] = acc
    attended = jnp.concatenate([att[pl.ds(h, 16, stride=NH), :] for h in range(NH)], axis=1).astype(BF16)

    pl.semaphore_wait(barrier, 4)
    y_copy = []
    for k in range(NY):
        y_send[k] = jnp.dot(attended, wo_ref[:, k * yw:(k + 1) * yw], preferred_element_type=F32)
        y_copy.append(remote(y_send.at[k], y_recv.at[k], y_ss.at[k], y_rs.at[k], other_tp))
        y_copy[k].start()
    for cp in in_copy:
        cp.wait()
    for k in range(NY):
        y_copy[k].wait()
        if k == 0:
            for cp in wd_copy:
                cp.start()
        cols = slice(k * yw, (k + 1) * yw)
        r_buf[:, cols] = x_buf[:, cols].astype(F32) + (y_send[k] + y_recv[k])
    normed = layer_norm(r_buf[...], g_buf[...]).astype(BF16)

    for k in range(NUP):
        wu_copy[k].wait()
        u = jnp.dot(normed, wu_buf[k], preferred_element_type=F32)
        hid[:, k * fw:(k + 1) * fw] = (0.5 * u * (1.0 + lax.erf(u * 0.5 ** 0.5))).astype(BF16)
    z_copy = []
    for k in range(NZ):
        wd_copy[k].wait()
        z_send[k] = jnp.dot(hid[...], wd_buf[k], preferred_element_type=F32)
        z_copy.append(remote(z_send.at[k], z_recv.at[k], z_ss.at[k], z_rs.at[k], other_tp))
        z_copy[k].start()

    def put(block, where, k):
        out_ref[pl.ds(pl.multiple_of(where * 16, 16), 16), k * zw:(k + 1) * zw] = block.astype(BF16)

    near, far, diag = [], [], []

    def arrived(k):
        far[k].wait()
        if k < NZ - 1:
            diag.append(remote(f_recv.at[1, k], f_recv.at[2, k], f_ss.at[2, k], f_rs.at[2, k], {"sp": sp_core}))
            diag[k].start()
        put(f_recv[1, k], sp_flip, k)

    for k in range(NZ):
        z_copy[k].wait()
        val = r_buf[:, k * zw:(k + 1) * zw] + (z_send[k] + z_recv[k])
        f_send[k] = val
        far.append(remote(f_send.at[k], f_recv.at[1, k], f_ss.at[1, k], f_rs.at[1, k], {"sp": sp_flip}))
        far[k].start()
        if k == NZ - 1:
            last = remote(f_send.at[k], f_recv.at[2, k], f_ss.at[2, k], f_rs.at[2, k], {"sp": sp_diag})
            last.start()
        near.append(remote(f_send.at[k], f_recv.at[0, k], f_ss.at[0, k], f_rs.at[0, k], {"sp": sp_core}))
        near[k].start()
        put(val, sp, k)
    for k in range(NZ):
        near[k].wait()
        put(f_recv[0, k], sp_core, k)
        arrived(k)
    diag.append(last)
    for k in range(NZ):
        diag[k].wait()
        put(f_recv[2, k], sp_diag, k)


def solution(mesh):
    def hbm(a):
        return pltpu.with_memory_space_constraint(a, pltpu.HBM)

    in_hbm = pl.BlockSpec(memory_space=pltpu.HBM)
    in_vmem = pl.BlockSpec(memory_space=pltpu.VMEM)
    dma = pltpu.SemaphoreType.DMA

    def local_layer(x_in, seq_lens, k_cache, v_cache, ln1_gain, w_qkv, w_out, ln2_gain, w_up, w_down):
        caches = [hbm(a.reshape(B, T * NH, HD)) for a in (k_cache, v_cache)]
        sp = lax.axis_index("sp")
        w_split, lhs = pl.pallas_call(
            prepare_kernel,
            out_shape=[pltpu.VMEM((12, D, 2, HD), BF16), pltpu.VMEM((2 * B, NQ), BF16)],
            in_specs=[in_hbm] * 3,
            out_specs=[in_vmem, in_vmem],
            scratch_shapes=[pltpu.VMEM((B, D), BF16), pltpu.VMEM((1, D), F32), dma((2,)), dma((12,))],
            compiler_params=pltpu.CompilerParams(vmem_limit_bytes=16 * 1024 * 1024),
            name="prepare",
        )(hbm(x_in), hbm(ln1_gain.reshape(1, D)), hbm(w_qkv.reshape(D, 12, 2, HD)))
        cache_shape = (B, T * NH, HD)
        ff = w_up.shape[1]
        k_upd, v_upd, parts = pl.pallas_call(
            attend_kernel,
            out_shape=[pltpu.VMEM(cache_shape, BF16), pltpu.VMEM(cache_shape, BF16),
                       jax.ShapeDtypeStruct((4, 144, HD), F32)],
            in_specs=[in_vmem] * 2 + [in_hbm] * 3,
            out_specs=[in_vmem] * 3,
            scratch_shapes=[
                pltpu.SMEM((B,), jnp.int32),
                pltpu.VMEM((B * NH, HD), F32), pltpu.VMEM((B * NH, HD), F32), pltpu.VMEM((B * NH, HD), F32),
                dma, dma((CH,)), dma((CH,)),
            ],
            compiler_params=pltpu.CompilerParams(vmem_limit_bytes=8 * 1024 * 1024),
            name="attend",
        )(lhs, w_split.reshape(12, NQ, HD), hbm(seq_lens), *caches)
        pieces = [lax.dynamic_index_in_dim(parts, (sp + rel) % 4, 0, keepdims=False) for rel in range(4)]
        moved = [lax.ppermute(pieces[rel], "sp", [(i, (i + rel) % 4) for i in range(4)]) for rel in (1, 2, 3)]
        k_next, v_next = pl.pallas_call(
            write_kernel,
            out_shape=[jax.ShapeDtypeStruct(cache_shape, BF16)] * 2,
            in_specs=[in_vmem] * 2,
            out_specs=[in_hbm] * 2,
            scratch_shapes=[dma((4,)), dma((4,))],
            compiler_params=pltpu.CompilerParams(vmem_limit_bytes=8 * 1024 * 1024),
            cost_estimate=pl.CostEstimate(flops=6 * 10 ** 9, bytes_accessed=16 << 20, transcendentals=0),
            name="write",
        )(k_upd, v_upd)
        x_out = pl.pallas_call(
            rest_kernel,
            out_shape=jax.ShapeDtypeStruct((B, D), BF16),
            in_specs=[in_vmem] * 5 + [in_hbm] * 4,
            out_specs=in_vmem,
            scratch_shapes=[
                pltpu.VMEM((16, D), BF16), pltpu.VMEM((1, D), F32),
                pltpu.VMEM((NUP, D, ff // NUP), BF16), pltpu.VMEM((NZ, ff, D // NZ), BF16),
                pltpu.VMEM((128, HD), F32),
                pltpu.VMEM((NY, 16, D // NY), F32), pltpu.VMEM((NY, 16, D // NY), F32),
                pltpu.VMEM((16, D), F32), pltpu.VMEM((16, ff), BF16),
                pltpu.VMEM((NZ, 16, D // NZ), F32), pltpu.VMEM((NZ, 16, D // NZ), F32),
                pltpu.VMEM((NZ, 16, D // NZ), F32), pltpu.VMEM((3, NZ, 16, D // NZ), F32),
                dma((2,)), dma((NUP,)), dma((NZ,)),
                dma((NY,)), dma((NY,)), dma((NZ,)), dma((NZ,)), dma((3, NZ)), dma((3, NZ)),
            ],
            compiler_params=pltpu.CompilerParams(vmem_limit_bytes=40 * 1024 * 1024, collective_id=0,
                                                 has_side_effects=True),
            cost_estimate=pl.CostEstimate(flops=10 ** 10, bytes_accessed=20 << 20, transcendentals=0),
            name="rest",
        )(pieces[0], *moved, w_out.reshape(NH * HD, D), hbm(x_in), hbm(ln2_gain.reshape(1, D)), hbm(w_up), hbm(w_down))
        return x_out, k_next.reshape(k_cache.shape), v_next.reshape(v_cache.shape)

    cache_spec = P("dp", "sp", "tp", None)
    in_specs = (P("dp", None), P("dp"), cache_spec, cache_spec, P(None), P(None, None, "tp", None), P("tp", None, None), P(None), P(None, "tp"), P("tp", None))
    out_specs = (P("dp", None), cache_spec, cache_spec)
    return jax.shard_map(local_layer, mesh=mesh, in_specs=in_specs, out_specs=out_specs, check_vma=False)
```

```python
import functools

import jax
import jax.numpy as jnp
from jax import lax
from jax.experimental import pallas as pl
from jax.experimental.pallas import tpu as pltpu
from jax.sharding import PartitionSpec as P

LN_EPS = 1e-5
NEG = -1e30
F32 = jnp.float32
BF16 = jnp.bfloat16
MESH = pl.DeviceIdType.MESH

B = 64
D = 2048
NH = 8
HD = 128
T = 64
NQ = 2 * D
CH = 4
CP = 32 // CH
AHEAD = 4
NUP = 1
NY = 4
NZ = 4


def layer_norm(x_f32, gain):
    mean = jnp.mean(x_f32, axis=-1, keepdims=True)
    centred = x_f32 - mean
    variance = jnp.mean(centred * centred, axis=-1, keepdims=True)
    return centred * lax.rsqrt(variance + LN_EPS) * gain


def prepare_kernel(x_hbm, g_hbm, w_hbm, w_out, lhs, x_buf, g_buf, small_sem, w_sem):
    small = [pltpu.make_async_copy(x_hbm, x_buf, small_sem.at[0]),
             pltpu.make_async_copy(g_hbm, g_buf, small_sem.at[1])]
    w_copy = [pltpu.make_async_copy(w_hbm.at[:, i], w_out.at[i], w_sem.at[i]) for i in range(12)]
    for c in small + w_copy:
        c.start()
    for c in small:
        c.wait()
    normed = layer_norm(x_buf[...].astype(F32), g_buf[...]).astype(BF16)
    spread = (lax.broadcasted_iota(jnp.int32, (128, 256), 1) // 2
              == lax.broadcasted_iota(jnp.int32, (128, 256), 0)).astype(BF16)
    odd = lax.broadcasted_iota(jnp.int32, (B, 256), 1) % 2 == 1
    for i in range(D // 128):
        twice = jnp.dot(normed[:, i * 128:(i + 1) * 128], spread, preferred_element_type=F32)
        lhs[0:B, i * 256:(i + 1) * 256] = jnp.where(odd, 0.0, twice).astype(BF16)
        lhs[B:2 * B, i * 256:(i + 1) * 256] = jnp.where(odd, twice, 0.0).astype(BF16)
    for c in w_copy:
        c.wait()


def attend_kernel(lhs, w_ref, lens_hbm, k_hbm, v_hbm, k_buf, v_buf, o_ref,
                  lens, q_s, k_s, v_s, small_sem, kin_sem, vin_sem):
    lens_copy = pltpu.make_async_copy(lens_hbm, lens, small_sem)
    lens_copy.start()

    def kv_in(i):
        at = pl.ds(i * 2 * CP, 2 * CP)
        return (pltpu.make_async_copy(k_hbm.at[at], k_buf.at[at], kin_sem.at[i]),
                pltpu.make_async_copy(v_hbm.at[at], v_buf.at[at], vin_sem.at[i]))

    for i in range(AHEAD):
        for c in kv_in(i):
            c.start()

    for i in range(0, 12, 2):
        two = jnp.concatenate([w_ref[i], w_ref[i + 1]], axis=1)
        res = jnp.dot(lhs[...], two, preferred_element_type=F32)
        for n in range(2):
            part, pair = divmod(i + n, 4)
            for parity in range(2):
                h = 2 * pair + parity
                val = res[parity * B:(parity + 1) * B, n * HD:(n + 1) * HD]
                (q_s, k_s, v_s)[part][pl.ds(h, B, stride=NH), :] = val
    lens_copy.wait()

    sp = lax.axis_index("sp")
    tp = lax.axis_index("tp")
    row = lax.broadcasted_iota(jnp.int32, (16, 1), 0)
    slope = jnp.exp2(-8.0 * (tp * NH + row % NH + 1).astype(F32) / (2 * NH))
    col = lax.broadcasted_iota(jnp.int32, (16, NH * T), 1)
    own_head = col % NH == lax.broadcasted_iota(jnp.int32, (16, NH * T), 0) % NH
    pos = jnp.where(own_head, sp * T + col // NH, 1 << 20)
    second = row >= 8
    upper = lax.broadcasted_iota(jnp.int32, (16, HD), 0) >= 8
    lane = lax.broadcasted_iota(jnp.int32, (16, HD), 1)

    def insert(buf, new, b):
        slot = lens[b] - sp * T
        held = jnp.logical_and(slot >= 0, slot < T)
        at = jnp.clip(slot, 0, T - 1)
        rows = pl.ds(pl.multiple_of((at // 2) * 16, 16), 16)
        fresh = new[pl.ds(pl.multiple_of(b * NH, NH), NH), :]
        fresh = jnp.concatenate([fresh, fresh], axis=0)
        keep = jnp.where(held, at % 2, 2)
        old = buf[b, rows, :].astype(F32)
        buf[b, rows, :] = jnp.where(upper.astype(jnp.int32) == keep, fresh, old).astype(BF16)

    def chunk(step, stats):
        for c in kv_in(step):
            c.wait()

        @pl.when(step + AHEAD < CH)
        def _():
            for c in kv_in(step + AHEAD):
                c.start()

        for n in range(2 * CP):
            insert(k_buf, k_s, step * 2 * CP + n)
            insert(v_buf, v_s, step * 2 * CP + n)
        scores = []
        for n in range(CP):
            j = step * CP + n
            q = q_s[pl.ds(pl.multiple_of(j * 16, 16), 16), :]
            q2 = jnp.concatenate([jnp.where(upper, 0.0, q), jnp.where(upper, q, 0.0)], axis=1).astype(BF16)
            k2 = jnp.concatenate([k_buf[2 * j], k_buf[2 * j + 1]], axis=1)
            scores.append(lax.dot_general(q2, k2, (((1,), (1,)), ((), ())), preferred_element_type=F32))
        weights = []
        for n in range(CP):
            j = step * CP + n
            length = jnp.where(second, lens[2 * j + 1], lens[2 * j])
            valid = pos <= length
            s = scores[n] * HD ** -0.5 - slope * (length - pos).astype(F32)
            s = jnp.where(valid, s, NEG)
            top = jnp.max(s, axis=1, keepdims=True)
            p = jnp.where(valid, jnp.exp(s - top), 0.0)
            total = jnp.sum(p, axis=1, keepdims=True)
            weights.append(p.astype(BF16))
            stats = jnp.where(lane == j, top, jnp.where(lane == 64 + j, total, stats))
        for n in range(CP):
            j = step * CP + n
            v2 = jnp.concatenate([v_buf[2 * j], v_buf[2 * j + 1]], axis=1)
            o = jnp.dot(weights[n], v2, preferred_element_type=F32)
            at = pl.multiple_of((j % 8) * 16, 16)
            o_ref[j // 8, pl.ds(at, 8), :] = o[0:8, :HD]
            o_ref[j // 8, pl.ds(at + 8, 8), :] = o[8:16, HD:]
        return stats

    stats = lax.fori_loop(0, CH, chunk, jnp.zeros((16, HD), F32))
    for i in range(4):
        o_ref[i, 128:144, :] = stats


def write_kernel(k_buf, v_buf, ko_hbm, vo_hbm, k_sem, v_sem):
    copies = []
    for i in range(4):
        at = pl.ds(i * (B // 4), B // 4)
        copies.append(pltpu.make_async_copy(k_buf.at[at], ko_hbm.at[at], k_sem.at[i]))
        copies.append(pltpu.make_async_copy(v_buf.at[at], vo_hbm.at[at], v_sem.at[i]))
    for c in copies:
        c.start()
    for c in copies:
        c.wait()


def rest_kernel(o0, o1, o2, o3, wo_ref, x_hbm, g_hbm, wu_hbm, wd_hbm, out_ref,
                x_buf, g_buf, wu_buf, wd_buf, att, y_send, y_recv, r_buf, hid, z_send, z_recv, f_send, f_recv,
                in_sem, wu_sem, wd_sem, y_ss, y_rs, z_ss, z_rs, f_ss, f_rs):
    sp = lax.axis_index("sp")
    tp = lax.axis_index("tp")
    x = sp // 2
    c = sp % 2
    sp_core = x * 2 + (1 - c)
    sp_flip = (1 - x) * 2 + c
    sp_diag = (1 - x) * 2 + (1 - c)
    other_tp = {"tp": 1 - tp}
    yw = D // NY
    fw = wu_hbm.shape[1] // NUP
    zw = D // NZ

    def remote(src, dst, ss, rs, dev):
        return pltpu.make_async_remote_copy(src_ref=src, dst_ref=dst, send_sem=ss, recv_sem=rs, device_id=dev,
                                            device_id_type=MESH)

    barrier = pltpu.get_barrier_semaphore()
    for dev in ({"sp": sp_core}, {"sp": sp_flip}, {"sp": sp_diag}, other_tp):
        pl.semaphore_signal(barrier, inc=1, device_id=dev, device_id_type=MESH)

    in_copy = [pltpu.make_async_copy(g_hbm, g_buf, in_sem.at[0]),
               pltpu.make_async_copy(x_hbm.at[pl.ds(pl.multiple_of(sp * 16, 16), 16)], x_buf, in_sem.at[1])]
    wu_copy = [pltpu.make_async_copy(wu_hbm.at[:, k * fw:(k + 1) * fw], wu_buf.at[k], wu_sem.at[k]) for k in range(NUP)]
    wd_copy = [pltpu.make_async_copy(wd_hbm.at[:, k * zw:(k + 1) * zw], wd_buf.at[k], wd_sem.at[k]) for k in range(NZ)]
    for cp in in_copy + wu_copy:
        cp.start()

    parts = [o0, o1, o2, o3]
    shift = lax.rem(HD - 8 * sp, HD)
    tops = [pltpu.roll(p[128:144, :], shift, 1) for p in parts]
    sums = [pltpu.roll(t, 64, 1) for t in tops]
    top = functools.reduce(jnp.maximum, tops)
    scale = [jnp.exp(t - top) for t in tops]
    total = functools.reduce(jnp.add, [a * s for a, s in zip(scale, sums)])
    scale = [a / total for a in scale]
    for j in range(8):
        acc = None
        for a, p in zip(scale, parts):
            term = p[j * 16:(j + 1) * 16, :] * a[:, j:j + 1]
            acc = term if acc is None else acc + term
        att[j * 16:(j + 1) * 16, :] = acc
    attended = jnp.concatenate([att[pl.ds(h, 16, stride=NH), :] for h in range(NH)], axis=1).astype(BF16)

    pl.semaphore_wait(barrier, 4)
    y_copy = []
    for k in range(NY):
        y_send[k] = jnp.dot(attended, wo_ref[:, k * yw:(k + 1) * yw], preferred_element_type=F32)
        y_copy.append(remote(y_send.at[k], y_recv.at[k], y_ss.at[k], y_rs.at[k], other_tp))
        y_copy[k].start()
    for cp in in_copy:
        cp.wait()
    for k in range(NY):
        y_copy[k].wait()
        if k == 0:
            for cp in wd_copy:
                cp.start()
        cols = slice(k * yw, (k + 1) * yw)
        r_buf[:, cols] = x_buf[:, cols].astype(F32) + (y_send[k] + y_recv[k])
    normed = layer_norm(r_buf[...], g_buf[...]).astype(BF16)

    for k in range(NUP):
        wu_copy[k].wait()
        u = jnp.dot(normed, wu_buf[k], preferred_element_type=F32)
        hid[:, k * fw:(k + 1) * fw] = (0.5 * u * (1.0 + lax.erf(u * 0.5 ** 0.5))).astype(BF16)
    z_copy = []
    for k in range(NZ):
        wd_copy[k].wait()
        z_send[k] = jnp.dot(hid[...], wd_buf[k], preferred_element_type=F32)
        z_copy.append(remote(z_send.at[k], z_recv.at[k], z_ss.at[k], z_rs.at[k], other_tp))
        z_copy[k].start()

    def put(block, where, k):
        out_ref[pl.ds(pl.multiple_of(where * 16, 16), 16), k * zw:(k + 1) * zw] = block.astype(BF16)

    near, far, diag = [], [], []

    def arrived(k):
        far[k].wait()
        if k < NZ - 1:
            diag.append(remote(f_recv.at[1, k], f_recv.at[2, k], f_ss.at[2, k], f_rs.at[2, k], {"sp": sp_core}))
            diag[k].start()
        put(f_recv[1, k], sp_flip, k)

    for k in range(NZ):
        z_copy[k].wait()
        val = r_buf[:, k * zw:(k + 1) * zw] + (z_send[k] + z_recv[k])
        f_send[k] = val
        far.append(remote(f_send.at[k], f_recv.at[1, k], f_ss.at[1, k], f_rs.at[1, k], {"sp": sp_flip}))
        far[k].start()
        if k == NZ - 1:
            last = remote(f_send.at[k], f_recv.at[2, k], f_ss.at[2, k], f_rs.at[2, k], {"sp": sp_diag})
            last.start()
        near.append(remote(f_send.at[k], f_recv.at[0, k], f_ss.at[0, k], f_rs.at[0, k], {"sp": sp_core}))
        near[k].start()
        put(val, sp, k)
    for k in range(NZ):
        near[k].wait()
        put(f_recv[0, k], sp_core, k)
        arrived(k)
    diag.append(last)
    for k in range(NZ):
        diag[k].wait()
        put(f_recv[2, k], sp_diag, k)


def solution(mesh):
    def hbm(a):
        return pltpu.with_memory_space_constraint(a, pltpu.HBM)

    in_hbm = pl.BlockSpec(memory_space=pltpu.HBM)
    in_vmem = pl.BlockSpec(memory_space=pltpu.VMEM)
    dma = pltpu.SemaphoreType.DMA

    def local_layer(x_in, seq_lens, k_cache, v_cache, ln1_gain, w_qkv, w_out, ln2_gain, w_up, w_down):
        caches = [hbm(a.reshape(B, T * NH, HD)) for a in (k_cache, v_cache)]
        sp = lax.axis_index("sp")
        w_split, lhs = pl.pallas_call(
            prepare_kernel,
            out_shape=[pltpu.VMEM((12, D, 2, HD), BF16), pltpu.VMEM((2 * B, NQ), BF16)],
            in_specs=[in_hbm] * 3,
            out_specs=[in_vmem, in_vmem],
            scratch_shapes=[pltpu.VMEM((B, D), BF16), pltpu.VMEM((1, D), F32), dma((2,)), dma((12,))],
            compiler_params=pltpu.CompilerParams(vmem_limit_bytes=16 * 1024 * 1024),
            name="prepare",
        )(hbm(x_in), hbm(ln1_gain.reshape(1, D)), hbm(w_qkv.reshape(D, 12, 2, HD)))
        cache_shape = (B, T * NH, HD)
        ff = w_up.shape[1]
        k_upd, v_upd, parts = pl.pallas_call(
            attend_kernel,
            out_shape=[pltpu.VMEM(cache_shape, BF16), pltpu.VMEM(cache_shape, BF16),
                       jax.ShapeDtypeStruct((4, 144, HD), F32)],
            in_specs=[in_vmem] * 2 + [in_hbm] * 3,
            out_specs=[in_vmem] * 3,
            scratch_shapes=[
                pltpu.SMEM((B,), jnp.int32),
                pltpu.VMEM((B * NH, HD), F32), pltpu.VMEM((B * NH, HD), F32), pltpu.VMEM((B * NH, HD), F32),
                dma, dma((CH,)), dma((CH,)),
            ],
            compiler_params=pltpu.CompilerParams(vmem_limit_bytes=8 * 1024 * 1024),
            name="attend",
        )(lhs, w_split.reshape(12, NQ, HD), hbm(seq_lens), *caches)
        pieces = [lax.dynamic_index_in_dim(parts, (sp + rel) % 4, 0, keepdims=False) for rel in range(4)]
        moved = [lax.ppermute(pieces[rel], "sp", [(i, (i + rel) % 4) for i in range(4)]) for rel in (1, 2, 3)]
        k_next, v_next = pl.pallas_call(
            write_kernel,
            out_shape=[jax.ShapeDtypeStruct(cache_shape, BF16)] * 2,
            in_specs=[in_vmem] * 2,
            out_specs=[in_hbm] * 2,
            scratch_shapes=[dma((4,)), dma((4,))],
            compiler_params=pltpu.CompilerParams(vmem_limit_bytes=8 * 1024 * 1024),
            cost_estimate=pl.CostEstimate(flops=6 * 10 ** 9, bytes_accessed=16 << 20, transcendentals=0),
            name="write",
        )(k_upd, v_upd)
        x_out = pl.pallas_call(
            rest_kernel,
            out_shape=jax.ShapeDtypeStruct((B, D), BF16),
            in_specs=[in_vmem] * 5 + [in_hbm] * 4,
            out_specs=in_vmem,
            scratch_shapes=[
                pltpu.VMEM((16, D), BF16), pltpu.VMEM((1, D), F32),
                pltpu.VMEM((NUP, D, ff // NUP), BF16), pltpu.VMEM((NZ, ff, D // NZ), BF16),
                pltpu.VMEM((128, HD), F32),
                pltpu.VMEM((NY, 16, D // NY), F32), pltpu.VMEM((NY, 16, D // NY), F32),
                pltpu.VMEM((16, D), F32), pltpu.VMEM((16, ff), BF16),
                pltpu.VMEM((NZ, 16, D // NZ), F32), pltpu.VMEM((NZ, 16, D // NZ), F32),
                pltpu.VMEM((NZ, 16, D // NZ), F32), pltpu.VMEM((3, NZ, 16, D // NZ), F32),
                dma((2,)), dma((NUP,)), dma((NZ,)),
                dma((NY,)), dma((NY,)), dma((NZ,)), dma((NZ,)), dma((3, NZ)), dma((3, NZ)),
            ],
            compiler_params=pltpu.CompilerParams(vmem_limit_bytes=40 * 1024 * 1024, collective_id=0,
                                                 has_side_effects=True),
            cost_estimate=pl.CostEstimate(flops=10 ** 10, bytes_accessed=20 << 20, transcendentals=0),
            name="rest",
        )(pieces[0], *moved, w_out.reshape(NH * HD, D), hbm(x_in), hbm(ln2_gain.reshape(1, D)), hbm(w_up), hbm(w_down))
        return x_out, k_next.reshape(k_cache.shape), v_next.reshape(v_cache.shape)

    cache_spec = P("dp", "sp", "tp", None)
    in_specs = (P("dp", None), P("dp"), cache_spec, cache_spec, P(None), P(None, None, "tp", None), P("tp", None, None), P(None), P(None, "tp"), P("tp", None))
    out_specs = (P("dp", None), cache_spec, cache_spec)
    return jax.shard_map(local_layer, mesh=mesh, in_specs=in_specs, out_specs=out_specs, check_vma=False)
```
